32 devices in a mesh: fsdp: 4 (over z), seq: 8 (over y, x, core).
Axes of the slice: x: 2, y: 2, z: 4, core: 2. Of those that a mesh axis runs over, the one named last changes fastest.
Arguments:
- timestep: int32 [4], P('fsdp'), may hold values from 0 to 999
- pooled: bfloat16 [4, 3072], P('fsdp'), may hold values from -6 to 6
- modulation_weight: bfloat16 [3072, 9216], P('fsdp', 'seq'), may hold values from -0.109375 to 0.109375
- reference_attention: bfloat16 [4, 2, 512, 1536], P('fsdp', None, 'seq'), may hold values from -6 to 6
- policy_attention: bfloat16 [4, 2, 512, 1536], P('fsdp', None, 'seq'), may hold values from -6 to 6
- reference_residual: bfloat16 [4, 2, 512, 3072], P('fsdp', None, 'seq'), may hold values from -6 to 6
- policy_residual: bfloat16 [4, 2, 512, 3072], P('fsdp', None, 'seq'), may hold values from -6 to 6
- noise: float32 [4, 2, 512, 64], P('fsdp', None, 'seq'), may hold values from -6 to 6
- latent: float32 [4, 2, 512, 64], P('fsdp', None, 'seq'), may hold values from -3 to 3
- frozen_output_weight: bfloat16 [1536, 3072], P(None, 'fsdp'), may hold values from -0.15625 to 0.15625
- adapter_down_weight: bfloat16 [64, 1536], P(None, 'fsdp'), may hold values from -0.15625 to 0.15625
- adapter_up_weight: bfloat16 [64, 3072], P(None, 'fsdp'), may hold values from -0.75 to 0.75
- reference_head: bfloat16 [64, 3072], P(None, 'fsdp'), may hold values from -0.109375 to 0.109375
- policy_head: bfloat16 [64, 3072], P(None, 'fsdp'), may hold values from -0.109375 to 0.109375
Outputs:
- loss: float32 [4], P('fsdp')
- grad_down: float32 [64, 1536], P(None, 'fsdp')
- grad_up: float32 [64, 3072], P(None, 'fsdp')
- grad_head: float32 [64, 3072], P(None, 'fsdp')
- grad_resid: bfloat16 [4, 2, 512, 3072], P('fsdp', None, 'seq')
- grad_attn: bfloat16 [4, 2, 512, 1536], P('fsdp', None, 'seq')
The draws below stay inside these ranges and needn't reach their ends.
All inputs are finite; a program needn't handle non-finite values.
Results may differ from the reference program's by a relative error of at most 0.029.
Values may be sent and summed in bfloat16 or wider, within the bound.
No kernel may reach another device: no remote copies, remote signals or barrier semaphores. Data moves between devices by JAX's collectives and lax.ppermute only.
A program may use at most 64 MiB of HBM per device.

```python
import math
import jax
import jax.numpy as jnp
from jax import lax

MODEL_WIDTH = 3072
CH = 64
HALF_FEATURES = 1536
ADAPTER_RANK = 64
LENGTH = 512
PAIRS = 4


def place_ends(drawn, stream_key, least, largest):
    shape = drawn.shape
    spot = [jax.random.randint(jax.random.fold_in(stream_key, axis), (), 0, shape[axis]) for axis in range(len(shape))]
    drawn = drawn.at[tuple(spot)].set(least)
    longest = shape.index(max(shape))
    spot[longest] = (spot[longest] + 1) % shape[longest]
    return drawn.at[tuple(spot)].set(largest)


def levels(own_key, shape, pieces, low, high):
    def one(axis_at, parts):
        steps = jax.random.uniform(jax.random.fold_in(jax.random.fold_in(own_key, 6), axis_at), (parts,), jnp.float32, low / len(pieces), high / len(pieces))
        return jnp.repeat(jnp.exp(steps), shape[axis_at] // parts).reshape((-1,) + (1,) * (len(shape) - axis_at - 1))

    level = one(*pieces[0])
    for cut in pieces[1:]:
        level = level * one(*cut)
    return level


def normal_values(own_key, dims, deviation, most, cuts=(), held_as=jnp.bfloat16):
    entries = jax.random.normal(own_key, dims, jnp.float32) * deviation
    if len(cuts) > 0:
        entries = levels(own_key, dims, cuts, -0.22, 0.18) * entries
    return jnp.clip(entries, min=-most, max=most).astype(held_as)


def setup_inputs(seed: int = 0) -> dict:
    seeds = jax.random.split(jax.random.key(seed), 15)
    return {
        "timestep": place_ends(jax.random.randint(seeds[0], (PAIRS,), 0, 1000), jax.random.fold_in(seeds[0], 1), 0, 999).astype(jnp.int32),
        "pooled": normal_values(seeds[1], (PAIRS, MODEL_WIDTH), 1.0, 6.0, ((0, 4),)),
        "modulation_weight": normal_values(seeds[2], (MODEL_WIDTH, 3 * MODEL_WIDTH), MODEL_WIDTH ** -0.5, 0.109375, ((0, 4), (1, 8))),
        "reference_attention": normal_values(seeds[3], (PAIRS, 2, LENGTH, HALF_FEATURES), 1.0, 6.0, ((0, 4), (2, 8))),
        "policy_attention": normal_values(seeds[4], (PAIRS, 2, LENGTH, HALF_FEATURES), 1.0, 6.0, ((0, 4), (2, 8))),
        "reference_residual": normal_values(seeds[5], (PAIRS, 2, LENGTH, MODEL_WIDTH), 1.0, 6.0, ((0, 4), (2, 8))),
        "policy_residual": normal_values(seeds[6], (PAIRS, 2, LENGTH, MODEL_WIDTH), 1.0, 6.0, ((0, 4), (2, 8))),
        "noise": normal_values(seeds[7], (PAIRS, 2, LENGTH, CH), 1.0, 6.0, ((0, 4), (2, 8)), jnp.float32),
        "latent": normal_values(seeds[8], (PAIRS, 2, LENGTH, CH), 0.5, 3.0, ((0, 4), (2, 8)), jnp.float32),
        "frozen_output_weight": normal_values(seeds[9], (HALF_FEATURES, MODEL_WIDTH), HALF_FEATURES ** -0.5, 0.15625, ((1, 4),)),
        "adapter_down_weight": normal_values(seeds[10], (ADAPTER_RANK, HALF_FEATURES), HALF_FEATURES ** -0.5, 0.15625, ((1, 4),)),
        "adapter_up_weight": normal_values(seeds[11], (ADAPTER_RANK, MODEL_WIDTH), ADAPTER_RANK ** -0.5, 0.75, ((1, 4),)),
        "reference_head": normal_values(seeds[12], (CH, MODEL_WIDTH), MODEL_WIDTH ** -0.5, 0.109375, ((1, 4),)),
        "policy_head": normal_values(seeds[13], (CH, MODEL_WIDTH), MODEL_WIDTH ** -0.5, 0.109375, ((1, 4),)),
    }


EPSILON = 1e-06

def embedding(timestep, layer_width):
    half_width = layer_width // 2
    frequency = jnp.exp(-math.log(10000.0) * jnp.arange(half_width, dtype=jnp.float32) / half_width)
    angles = timestep.astype(jnp.float32)[:, None] * frequency[None, :]
    return jnp.concatenate([jnp.cos(angles), jnp.sin(angles)], axis=1)

def contract_rows(left, right):
    return lax.dot_general(left, right, (((0,), (0,)), ((), ())), preferred_element_type=jnp.float32)

def contracted_columns(left, right):
    return lax.dot_general(left, right, (((1,), (1,)), ((), ())), preferred_element_type=jnp.float32)

def final_layer(projected, residual, gate_row, shift_row, scale_row, head):
    stream = residual.astype(jnp.float32) + gate_row * projected
    row_mean = lax.optimization_barrier(jnp.mean(stream, axis=1, keepdims=True))
    centred = stream - row_mean
    variance = lax.optimization_barrier(jnp.mean(centred * centred, axis=1, keepdims=True))
    inv_std = lax.rsqrt(variance + EPSILON)
    normed = centred * inv_std
    modulated = (normed * (1.0 + scale_row) + shift_row).astype(jnp.bfloat16)
    predicted = contracted_columns(modulated, head)
    return (normed, inv_std, modulated, predicted)

def member_errors(predicted, target, scale_total):
    offset = predicted - target
    squared = lax.optimization_barrier(jnp.sum(offset * offset, axis=1))
    return lax.optimization_barrier(jnp.sum(squared.reshape(2, -1), axis=1)) / scale_total

def reference(timestep, pooled, modulation_weight, reference_attention, policy_attention, reference_residual, policy_residual, noise, latent, frozen_output_weight, adapter_down_weight, adapter_up_weight, reference_head, policy_head):
    layer_width = pooled.shape[1]
    feature_index = reference_attention.shape[-1]
    channel_count = noise.shape[-1]
    length = reference_attention.shape[2]
    scale_total = float(length * channel_count)
    beta = math.sqrt(length * channel_count) / 8.0
    cond_vec = pooled.astype(jnp.float32) + embedding(timestep, layer_width)
    activated = jax.nn.silu(cond_vec).astype(jnp.bfloat16)
    modulation = jnp.dot(activated, modulation_weight, preferred_element_type=jnp.float32)
    sign_rows = jnp.concatenate([jnp.ones((length, 1), jnp.float32), -jnp.ones((length, 1), jnp.float32)], axis=0)

    def one_pair(items):
        mod_row, pair_attn_ref, pair_attn_pol, pair_resid_ref, pair_resid_pol, pair_noise, pair_latent = items
        gate_row = mod_row[None, :layer_width]
        shift_row = mod_row[None, layer_width:2 * layer_width]
        scale_row = mod_row[None, 2 * layer_width:]
        rows_ref = pair_attn_ref.reshape(-1, feature_index)
        policy_rows = pair_attn_pol.reshape(-1, feature_index)
        stream_ref = pair_resid_ref.reshape(-1, layer_width)
        stream_pol = pair_resid_pol.reshape(-1, layer_width)
        target = (pair_noise - pair_latent).reshape(-1, channel_count)
        proj_ref = jnp.dot(rows_ref, frozen_output_weight, preferred_element_type=jnp.float32)
        normed_ref, inv_ref, z_ref, pred_ref = final_layer(proj_ref, stream_ref, gate_row, shift_row, scale_row, reference_head)
        err_ref = member_errors(pred_ref, target, scale_total)
        low_rank_rows = contracted_columns(policy_rows, adapter_down_weight).astype(jnp.bfloat16)
        policy_projection = jnp.dot(policy_rows, frozen_output_weight, preferred_element_type=jnp.float32) + jnp.dot(low_rank_rows, adapter_up_weight, preferred_element_type=jnp.float32)
        normed_pol, inv_pol, z_pol, pred_pol = final_layer(policy_projection, stream_pol, gate_row, shift_row, scale_row, policy_head)
        err_pol = member_errors(pred_pol, target, scale_total)
        margin = err_pol[0] - err_ref[0] - (err_pol[1] - err_ref[1])
        loss_pair = jax.nn.softplus(beta * margin)
        weight_pair = jax.nn.sigmoid(beta * margin)
        dpred = (sign_rows * weight_pair * 2.0 * (pred_pol - target)).astype(jnp.bfloat16)
        head_part = contract_rows(dpred, z_pol)
        dz_rows = jnp.dot(dpred, policy_head, preferred_element_type=jnp.float32)
        dn_rows = dz_rows * (1.0 + scale_row)
        dstream = inv_pol * (dn_rows - lax.optimization_barrier(jnp.mean(dn_rows, axis=1, keepdims=True)) - normed_pol * lax.optimization_barrier(jnp.mean(dn_rows * normed_pol, axis=1, keepdims=True)))
        resid_grad = dstream.astype(jnp.bfloat16)
        projection_gradient = (gate_row * dstream).astype(jnp.bfloat16)
        up_part = contract_rows(low_rank_rows, projection_gradient)
        low_rank_gradient = contracted_columns(projection_gradient, adapter_up_weight).astype(jnp.bfloat16)
        down_part = contract_rows(low_rank_gradient, policy_rows)
        attention_gradient = (contracted_columns(projection_gradient, frozen_output_weight) + jnp.dot(low_rank_gradient, adapter_down_weight, preferred_element_type=jnp.float32)).astype(jnp.bfloat16)
        return (loss_pair, resid_grad, attention_gradient, down_part, up_part, head_part)
    results = lax.map(one_pair, (modulation, reference_attention, policy_attention, reference_residual, policy_residual, noise, latent))
    loss = results[0]
    down_sum = lax.optimization_barrier(jnp.sum(results[3], axis=0))
    up_sum = lax.optimization_barrier(jnp.sum(results[4], axis=0))
    head_sum = lax.optimization_barrier(jnp.sum(results[5], axis=0))
    total = jnp.sum(down_sum * down_sum) + jnp.sum(up_sum * up_sum) + jnp.sum(head_sum * head_sum)
    upper_limit = math.sqrt(down_sum.size + up_sum.size + head_sum.size)
    factor = jnp.minimum(1.0, upper_limit / jnp.sqrt(total + 1e-12))
    grad_resid = results[1].reshape(policy_residual.shape)
    grad_attn = results[2].reshape(policy_attention.shape)
    return (loss, factor * down_sum, factor * up_sum, factor * head_sum, grad_resid, grad_attn)
```

```python
import math

import jax
import jax.numpy as jnp
from jax import lax
from jax.sharding import PartitionSpec as P

EPSILON = 1e-06


def embedding(timestep, layer_width):
    half_width = layer_width // 2
    frequency = jnp.exp(-math.log(10000.0) * jnp.arange(half_width, dtype=jnp.float32) / half_width)
    angles = timestep.astype(jnp.float32)[:, None] * frequency[None, :]
    return jnp.concatenate([jnp.cos(angles), jnp.sin(angles)], axis=1)


def contract_rows(left, right):
    return lax.dot_general(
        left, right, (((0,), (0,)), ((), ())), preferred_element_type=jnp.float32
    )


def contracted_columns(left, right):
    return lax.dot_general(
        left, right, (((1,), (1,)), ((), ())), preferred_element_type=jnp.float32
    )


def shift(value, step):
    count = lax.axis_size("fsdp")
    return lax.ppermute(value, "fsdp", [(i, (i + step) % count) for i in range(count)])


def swap(value, mask):
    count = lax.axis_size("seq")
    return lax.ppermute(value, "seq", [(i, i ^ mask) for i in range(count)])


def pick(value, index, axis=0):
    return lax.dynamic_index_in_dim(value, index, axis, keepdims=False)


def in_order(pieces, index):
    stacked = jnp.stack(pieces)
    places = [pick(stacked, index ^ place) for place in range(len(pieces))]
    return jnp.stack(places)


def gather_seq(value, seq_index):
    count = lax.axis_size("seq")
    plane = [value] + [swap(value, 2 * mask) for mask in range(1, count // 2)]
    stacked = jnp.stack(plane)
    other = swap(stacked, 1)
    both = []
    for mask in range(count // 2):
        both += [stacked[mask], other[mask]]
    return in_order(both, seq_index)


def final_layer(projected, residual, gate_row, shift_row, scale_row, head):
    stream = residual.astype(jnp.float32) + gate_row * projected
    row_mean = jnp.mean(stream, axis=1, keepdims=True)
    centred = stream - row_mean
    variance = jnp.mean(centred * centred, axis=1, keepdims=True)
    inv_std = lax.rsqrt(variance + EPSILON)
    normed = centred * inv_std
    modulated = (normed * (1.0 + scale_row) + shift_row).astype(jnp.bfloat16)
    predicted = contracted_columns(modulated, head)
    return (normed, inv_std, modulated, predicted)


def member_errors(predicted, target, scale_total):
    offset = predicted - target
    squared = jnp.sum(offset * offset, axis=1)
    return jnp.sum(squared.reshape(2, -1), axis=1) / scale_total


def gather_weights(ext, fsdp_index, seq_index):
    rows, columns = ext.shape
    count_f, count_s = lax.axis_size("fsdp"), lax.axis_size("seq")
    part = rows // count_s
    chunk = lax.dynamic_slice(ext, (seq_index * part, 0), (part, columns))
    full = jnp.zeros((rows, columns * count_f), ext.dtype)
    full = lax.dynamic_update_slice(full, ext, (0, fsdp_index * columns))
    arrived = [shift(chunk, step) for step in range(1, count_f)]
    group = -(-len(arrived) // 3)
    for first in range(1, count_f, group):
        steps = range(first, min(first + group, count_f))
        own = jnp.concatenate([arrived[step - 1] for step in steps], axis=0)
        plane = [own] + [swap(own, 2 * mask) for mask in range(1, count_s // 2)]
        pieces = []
        for piece in plane:
            pieces += [piece, swap(piece, 1)]

        def place(at, full, piece, mask):
            row = (seq_index ^ mask) * part
            column = ((fsdp_index - first - at) % count_f) * columns
            held = lax.dynamic_slice(piece, (at * part, 0), (part, columns))
            return lax.dynamic_update_slice(full, held, (row, column))

        for mask, piece in enumerate(pieces):
            if group == 1:
                full = place(0, full, piece, mask)
            else:
                full = lax.fori_loop(
                    0, len(steps), lambda at, held: place(at, held, piece, mask), full
                )
    return full


def local(
    timestep,
    pooled,
    modulation_weight,
    reference_attention,
    policy_attention,
    reference_residual,
    policy_residual,
    noise,
    latent,
    frozen_output_weight,
    adapter_down_weight,
    adapter_up_weight,
    reference_head,
    policy_head,
):
    layer_width = pooled.shape[1]
    feature_index = reference_attention.shape[-1]
    channel_count = noise.shape[-1]
    rank = adapter_down_weight.shape[0]
    tok_seq = reference_attention.shape[2]
    count_f, count_s = lax.axis_size("fsdp"), lax.axis_size("seq")
    fsdp_index, seq_index = lax.axis_index("fsdp"), lax.axis_index("seq")
    length = tok_seq * count_s
    scale_total = float(length * channel_count)
    beta = math.sqrt(length * channel_count) / 8.0

    cond_vec = pooled.astype(jnp.float32) + embedding(timestep, layer_width)
    activated = jax.nn.silu(cond_vec).astype(jnp.bfloat16)
    by_block = activated.reshape(pooled.shape[0], count_f, -1).transpose(1, 0, 2)
    pieces = [pick(by_block, fsdp_index)]
    for step in range(1, count_f):
        pieces.append(shift(pick(by_block, (fsdp_index + step) % count_f), step))
    per_pair = pooled.shape[0]
    partial_value = jnp.dot(
        jnp.concatenate(pieces, axis=0), modulation_weight, preferred_element_type=jnp.float32
    )
    own_part = partial_value[:per_pair]
    for step in range(1, count_f):
        own_part = own_part + shift(
            partial_value[per_pair * step : per_pair * (step + 1)], count_f - step
        )
    modulation = gather_seq(own_part, seq_index).transpose(1, 0, 2).reshape(per_pair, -1)
    gate_row = modulation[:, :layer_width]
    shift_row = modulation[:, layer_width : 2 * layer_width]
    scale_row = modulation[:, 2 * layer_width :]

    block = frozen_output_weight.shape[1]
    down_block = adapter_down_weight.shape[1]
    ext = jnp.concatenate(
        [
            frozen_output_weight,
            adapter_up_weight,
            reference_head,
            policy_head,
            jnp.pad(adapter_down_weight, ((0, 0), (0, block - down_block))),
        ],
        axis=0,
    )
    full = gather_weights(ext, fsdp_index, seq_index)
    base_full = full[:feature_index]
    up_full = full[feature_index : feature_index + rank]
    head_ref_full = full[feature_index + rank : feature_index + rank + channel_count]
    head_pol_full = full[feature_index + rank + channel_count : feature_index + rank + 2 * channel_count]
    down_full = (
        full[feature_index + rank + 2 * channel_count :]
        .reshape(rank, count_f, block)[:, :, :down_block]
        .reshape(rank, feature_index)
    )

    rows_ref = reference_attention.reshape(-1, feature_index)
    policy_rows = policy_attention.reshape(-1, feature_index)
    stream_ref = reference_residual.reshape(-1, layer_width)
    stream_pol = policy_residual.reshape(-1, layer_width)
    target = (noise - latent).reshape(-1, channel_count)
    sign_rows = jnp.concatenate(
        [jnp.ones((tok_seq, 1), jnp.float32), -jnp.ones((tok_seq, 1), jnp.float32)], axis=0
    )
    proj_ref = jnp.dot(rows_ref, base_full, preferred_element_type=jnp.float32)
    normed_ref, inv_ref, z_ref, pred_ref = final_layer(
        proj_ref, stream_ref, gate_row, shift_row, scale_row, head_ref_full
    )
    part_ref = member_errors(pred_ref, target, scale_total)
    low_rank_rows = contracted_columns(policy_rows, down_full).astype(jnp.bfloat16)
    policy_projection = jnp.dot(
        policy_rows, base_full, preferred_element_type=jnp.float32
    ) + jnp.dot(low_rank_rows, up_full, preferred_element_type=jnp.float32)
    normed_pol, inv_pol, z_pol, pred_pol = final_layer(
        policy_projection, stream_pol, gate_row, shift_row, scale_row, head_pol_full
    )
    part_pol = member_errors(pred_pol, target, scale_total)
    local_margin = part_pol[0] - part_ref[0] - (part_pol[1] - part_ref[1])
    margin_row = jnp.full((8, 128), local_margin, jnp.float32)
    margin = jnp.sum(gather_seq(margin_row, seq_index)[:, 0, 0])
    loss = jax.nn.softplus(beta * margin).reshape(1)
    weight_pair = jax.nn.sigmoid(beta * margin)

    dpred = (sign_rows * 2.0 * (pred_pol - target)).astype(jnp.bfloat16)
    head_part = contract_rows(dpred, z_pol)
    dz_rows = jnp.dot(dpred, head_pol_full, preferred_element_type=jnp.float32)
    dn_rows = dz_rows * (1.0 + scale_row)
    dstream = inv_pol * (
        dn_rows
        - jnp.mean(dn_rows, axis=1, keepdims=True)
        - normed_pol * jnp.mean(dn_rows * normed_pol, axis=1, keepdims=True)
    )
    projection_gradient = (gate_row * dstream).astype(jnp.bfloat16)
    up_part = contract_rows(low_rank_rows, projection_gradient)
    low_rank_gradient = contracted_columns(projection_gradient, up_full).astype(jnp.bfloat16)
    down_part = contract_rows(low_rank_gradient, policy_rows)
    grad_resid = (weight_pair * dstream).astype(jnp.bfloat16).reshape(policy_residual.shape)
    grad_attn = (
        (
            weight_pair
            * (
                contracted_columns(projection_gradient, base_full)
                + jnp.dot(low_rank_gradient, down_full, preferred_element_type=jnp.float32)
            )
        )
        .astype(jnp.bfloat16)
        .reshape(policy_attention.shape)
    )

    def blocks(value):
        return value.astype(jnp.bfloat16).reshape(value.shape[0], count_f, -1).transpose(1, 0, 2)

    grads = jnp.concatenate([blocks(down_part), blocks(up_part), blocks(head_part)], axis=2)
    width = grads.shape[2]
    plane_count = count_s // 2
    plane_index, core = seq_index // 2, seq_index % 2
    grads = grads.reshape(count_f, plane_count, 2, rank // count_s, width)
    mine = pick(grads, core, 2)
    theirs = swap(pick(grads, 1 - core, 2), 1)
    half = (mine.astype(jnp.float32) + theirs.astype(jnp.float32)).astype(jnp.bfloat16)
    total = pick(half, plane_index, 1).astype(jnp.float32)
    for mask in range(1, plane_count):
        total = total + swap(pick(half, plane_index ^ mask, 1), 2 * mask).astype(jnp.float32)
    pair_sum = (weight_pair * total).astype(jnp.bfloat16)
    own_sum = pick(pair_sum, fsdp_index).astype(jnp.float32)
    for step in range(1, count_f):
        own_sum = own_sum + shift(pick(pair_sum, (fsdp_index + step) % count_f), step).astype(
            jnp.float32
        )
    gathered = gather_seq(own_sum.astype(jnp.bfloat16), seq_index)
    sums = gathered.reshape(rank, width).astype(jnp.float32)
    square = jnp.full((8, 128), jnp.sum(sums * sums), jnp.float32)
    total_square = square
    for step in range(1, count_f):
        total_square = total_square + shift(square, step)
    upper_limit = math.sqrt(
        rank * feature_index + rank * layer_width + channel_count * layer_width
    )
    factor = jnp.minimum(1.0, upper_limit / jnp.sqrt(total_square[0, 0] + 1e-12))
    scaled = factor * sums
    return (
        loss,
        scaled[:, :down_block],
        scaled[:, down_block : down_block + block],
        scaled[:, down_block + block :],
        grad_resid,
        grad_attn,
    )


def solution(mesh):
    in_specs = (
        P("fsdp"),
        P("fsdp", None),
        P("fsdp", "seq"),
        P("fsdp", None, "seq", None),
        P("fsdp", None, "seq", None),
        P("fsdp", None, "seq", None),
        P("fsdp", None, "seq", None),
        P("fsdp", None, "seq", None),
        P("fsdp", None, "seq", None),
        P(None, "fsdp"),
        P(None, "fsdp"),
        P(None, "fsdp"),
        P(None, "fsdp"),
        P(None, "fsdp"),
    )
    out_specs = (
        P("fsdp"),
        P(None, "fsdp"),
        P(None, "fsdp"),
        P(None, "fsdp"),
        P("fsdp", None, "seq", None),
        P("fsdp", None, "seq", None),
    )
    return jax.shard_map(local, mesh=mesh, in_specs=in_specs, out_specs=out_specs, check_vma=False)
```

```python
import math

import jax
import jax.numpy as jnp
from jax import lax
from jax.experimental import pallas as pl
from jax.experimental.pallas import tpu as pltpu
from jax.sharding import PartitionSpec as P

EPSILON = 1e-06


def embedding(timestep, layer_width):
    half_width = layer_width // 2
    frequency = jnp.exp(-math.log(10000.0) * jnp.arange(half_width, dtype=jnp.float32) / half_width)
    angles = timestep.astype(jnp.float32)[:, None] * frequency[None, :]
    return jnp.concatenate([jnp.cos(angles), jnp.sin(angles)], axis=1)


def contract_rows(left, right):
    return lax.dot_general(
        left, right, (((0,), (0,)), ((), ())), preferred_element_type=jnp.float32
    )


def contracted_columns(left, right):
    return lax.dot_general(
        left, right, (((1,), (1,)), ((), ())), preferred_element_type=jnp.float32
    )


def shift(value, step):
    count = lax.axis_size("fsdp")
    return lax.ppermute(value, "fsdp", [(i, (i + step) % count) for i in range(count)])


def swap(value, mask):
    count = lax.axis_size("seq")
    return lax.ppermute(value, "seq", [(i, i ^ mask) for i in range(count)])


def pick(value, index, axis=0):
    return lax.dynamic_index_in_dim(value, index, axis, keepdims=False)


def in_order(pieces, index):
    stacked = jnp.stack(pieces)
    places = [pick(stacked, index ^ place) for place in range(len(pieces))]
    return jnp.stack(places)


def gather_seq(value, seq_index):
    count = lax.axis_size("seq")
    plane = [value] + [swap(value, 2 * mask) for mask in range(1, count // 2)]
    stacked = jnp.stack(plane)
    other = swap(stacked, 1)
    both = []
    for mask in range(count // 2):
        both += [stacked[mask], other[mask]]
    return in_order(both, seq_index)


def final_layer(projected, residual, gate_row, shift_row, scale_row, head):
    stream = residual.astype(jnp.float32) + gate_row * projected
    row_mean = jnp.mean(stream, axis=1, keepdims=True)
    centred = stream - row_mean
    variance = jnp.mean(centred * centred, axis=1, keepdims=True)
    inv_std = lax.rsqrt(variance + EPSILON)
    normed = centred * inv_std
    modulated = (normed * (1.0 + scale_row) + shift_row).astype(jnp.bfloat16)
    predicted = contracted_columns(modulated, head)
    return (normed, inv_std, modulated, predicted)


def member_errors(predicted, target, scale_total):
    offset = predicted - target
    squared = jnp.sum(offset * offset, axis=1)
    return jnp.sum(squared.reshape(2, -1), axis=1) / scale_total


def gather_weights(ext, fsdp_index, seq_index):
    rows, columns = ext.shape
    count_f, count_s = lax.axis_size("fsdp"), lax.axis_size("seq")
    part = rows // count_s
    chunk = lax.dynamic_slice(ext, (seq_index * part, 0), (part, columns))
    full = jnp.zeros((rows, columns * count_f), ext.dtype)
    full = lax.dynamic_update_slice(full, ext, (0, fsdp_index * columns))
    arrived = [shift(chunk, step) for step in range(1, count_f)]
    group = -(-len(arrived) // 3)
    for first in range(1, count_f, group):
        steps = range(first, min(first + group, count_f))
        own = jnp.concatenate([arrived[step - 1] for step in steps], axis=0)
        plane = [own] + [swap(own, 2 * mask) for mask in range(1, count_s // 2)]
        pieces = []
        for piece in plane:
            pieces += [piece, swap(piece, 1)]

        def place(at, full, piece, mask):
            row = (seq_index ^ mask) * part
            column = ((fsdp_index - first - at) % count_f) * columns
            held = lax.dynamic_slice(piece, (at * part, 0), (part, columns))
            return lax.dynamic_update_slice(full, held, (row, column))

        for mask, piece in enumerate(pieces):
            if group == 1:
                full = place(0, full, piece, mask)
            else:
                full = lax.fori_loop(
                    0, len(steps), lambda at, held: place(at, held, piece, mask), full
                )
    return full


def dot(left, right):
    return jnp.dot(left, right, preferred_element_type=jnp.float32)


def step_kernel(sizes, where, *refs):
    tokens, features, width, rank, channels, count_f, count_s, scale_total = sizes
    block, down_block = width // count_f, features // count_f
    part, small_part = features // count_s, (2 * rank + 2 * channels) // count_s
    (attn_pol, attn_ref, res_pol, res_ref, noise, latent, mod, own, own_small), refs = refs[:9], refs[9:]
    chunks, refs = refs[: (count_f - 1) * count_s], refs[(count_f - 1) * count_s :]
    keep, send, margin_out, dstream_out, attn_out, refs = *refs[:5], refs[5:]
    rows, base, small, residual, proj, z_hold, back, dproj, sems = refs
    fsdp_index, seq_index = where[0], where[1]

    def start(source, target, slot):
        copy = pltpu.make_async_copy(source, target, sems.at[slot])
        copy.start()
        return copy

    first = [
        start(attn_pol, rows.at[:tokens], 0),
        start(attn_ref, rows.at[tokens:], 1),
    ]
    blocks = [[start(own, base.at[fsdp_index], 2)]]
    smalls = [start(own_small, small.at[fsdp_index], 3)]
    slot = 6
    for step in range(1, count_f):
        at = lax.rem(fsdp_index - step + count_f, count_f)
        waits = []
        for mask in range(count_s):
            chunk = chunks[(step - 1) * count_s + mask]
            place = lax.bitwise_xor(seq_index, mask)
            waits.append(
                start(
                    chunk.at[:part],
                    base.at[at, pl.ds(pl.multiple_of(place * part, part), part)],
                    slot,
                )
            )
            smalls.append(
                start(
                    chunk.at[part:],
                    small.at[at, pl.ds(pl.multiple_of(place * small_part, small_part), small_part)],
                    slot + 1,
                )
            )
            slot += 2
        blocks.append(waits)
    late = [
        start(res_pol, residual.at[:tokens], 4),
        start(res_ref, residual.at[tokens:], 5),
    ]
    for copy in first:
        copy.wait()
    for step in range(count_f):
        for copy in blocks[step]:
            copy.wait()
        at = lax.rem(fsdp_index - step + count_f, count_f)
        proj[at] = dot(rows[...], base[at])
    for copy in smalls + late:
        copy.wait()

    def up_of(g):
        return small[g, :rank]

    def head_of(g, policy):
        first_row = rank + (channels if policy else 0)
        return small[g, first_row : first_row + channels]

    def down_of(g):
        return small[g, rank + 2 * channels :, :down_block]

    def columns(g):
        return slice(g * block, (g + 1) * block)

    def gate_of(g):
        return mod[:, g * block : (g + 1) * block]

    def shift_of(g):
        return mod[:, width + g * block : width + (g + 1) * block]

    def scale_of(g):
        return 1.0 + mod[:, 2 * width + g * block : 2 * width + (g + 1) * block]

    low = jnp.zeros((tokens, rank), jnp.float32)
    for g in range(count_f):
        low = low + contracted_columns(
            rows[:tokens, g * down_block : (g + 1) * down_block], down_of(g)
        )
    low_rows = low.astype(jnp.bfloat16)
    row_sum = jnp.zeros((2 * tokens, 1), jnp.float32)
    for g in range(count_f):
        proj[g, :tokens] = proj[g, :tokens] + dot(low_rows, up_of(g))
        stream = residual[:, columns(g)].astype(jnp.float32) + gate_of(g) * proj[g]
        proj[g] = stream
        row_sum = row_sum + jnp.sum(stream, axis=1, keepdims=True)
    mean = row_sum / width
    square_sum = jnp.zeros((2 * tokens, 1), jnp.float32)
    for g in range(count_f):
        centred = proj[g] - mean
        square_sum = square_sum + jnp.sum(centred * centred, axis=1, keepdims=True)
    inv_std = lax.rsqrt(square_sum / width + EPSILON)
    pred_pol = jnp.zeros((tokens, channels), jnp.float32)
    pred_ref = jnp.zeros((tokens, channels), jnp.float32)
    for g in range(count_f):
        normed = (proj[g] - mean) * inv_std
        proj[g] = normed
        z_rows = (normed * scale_of(g) + shift_of(g)).astype(jnp.bfloat16)
        z_hold[g] = z_rows[:tokens]
        pred_pol = pred_pol + contracted_columns(z_rows[:tokens], head_of(g, True))
        pred_ref = pred_ref + contracted_columns(z_rows[tokens:], head_of(g, False))
    target = noise[...] - latent[...]
    half_rows = lax.broadcasted_iota(jnp.int32, (tokens, channels), 0) < tokens // 2
    sign = jnp.where(half_rows, 1.0, -1.0)
    off_pol, off_ref = pred_pol - target, pred_ref - target
    margin_out[...] = jnp.full(
        margin_out.shape,
        jnp.sum(sign * (off_pol * off_pol - off_ref * off_ref)) / scale_total,
        jnp.float32,
    )
    dpred_wide = 2.0 * sign * off_pol
    dpred = dpred_wide.astype(jnp.bfloat16)
    dpred_turned = dpred_wide.T.astype(jnp.bfloat16)
    low_turned = low.T.astype(jnp.bfloat16)
    sum_dn = jnp.zeros((tokens, 1), jnp.float32)
    sum_dn_normed = jnp.zeros((tokens, 1), jnp.float32)
    half = rank // 2
    core = lax.rem(seq_index, 2)

    def put(g, first_column, value):
        value = value.astype(jnp.bfloat16).astype(jnp.float32)
        last_column = first_column + value.shape[1]
        top, bottom = value[:half], value[half:]
        keep[g, :, first_column:last_column] = jnp.where(core == 0, top, bottom).astype(jnp.bfloat16)
        send[g, :, first_column:last_column] = jnp.where(core == 0, bottom, top).astype(jnp.bfloat16)

    for g in range(count_f):
        put(g, down_block + block, dot(dpred_turned, z_hold[g]))
        dn_rows = dot(dpred, head_of(g, True)) * scale_of(g)
        back[g] = dn_rows
        sum_dn = sum_dn + jnp.sum(dn_rows, axis=1, keepdims=True)
        sum_dn_normed = sum_dn_normed + jnp.sum(dn_rows * proj[g, :tokens], axis=1, keepdims=True)
    mean_dn, mean_dn_normed = sum_dn / width, sum_dn_normed / width
    inv_pol = inv_std[:tokens]
    low_grad = jnp.zeros((tokens, rank), jnp.float32)
    for g in range(count_f):
        dstream = inv_pol * (back[g] - mean_dn - proj[g, :tokens] * mean_dn_normed)
        dstream_out[:, columns(g)] = dstream
        dproj_rows = (gate_of(g) * dstream).astype(jnp.bfloat16)
        dproj[g] = dproj_rows
        put(g, down_block, dot(low_turned, dproj_rows))
        low_grad = low_grad + contracted_columns(dproj_rows, up_of(g))
    low_grad_rows = low_grad.astype(jnp.bfloat16)
    low_grad_turned = low_grad.T.astype(jnp.bfloat16)
    for g in range(count_f):
        put(g, 0, dot(low_grad_turned, rows[:tokens, g * down_block : (g + 1) * down_block]))
    for g in range(count_f):
        at = slice(g * down_block, (g + 1) * down_block)
        value = dot(low_grad_rows, down_of(g))
        for other in range(count_f):
            value = value + contracted_columns(dproj[other], base[other, at])
        attn_out[:, at] = value


def step_call(where, operands, chunks, tokens, features, width, rank, channels, scale_total):
    count_f, count_s = lax.axis_size("fsdp"), lax.axis_size("seq")
    sizes = (tokens, features, width, rank, channels, count_f, count_s, scale_total)
    block = width // count_f
    grads = jax.ShapeDtypeStruct(
        (count_f, rank // 2, features // count_f + 2 * block), jnp.bfloat16
    )
    any_space = pl.BlockSpec(memory_space=pl.ANY)
    vmem = pl.BlockSpec(memory_space=pltpu.VMEM)
    return pl.pallas_call(
        lambda *refs: step_kernel(sizes, *refs),
        out_shape=(
            grads,
            grads,
            jax.ShapeDtypeStruct((8, 128), jnp.float32),
            jax.ShapeDtypeStruct((tokens, width), jnp.float32),
            jax.ShapeDtypeStruct((tokens, features), jnp.float32),
        ),
        in_specs=[pl.BlockSpec(memory_space=pltpu.SMEM)]
        + [any_space] * 4
        + [vmem] * 3
        + [any_space] * (2 + len(chunks)),
        out_specs=(vmem,) * 5,
        scratch_shapes=[
            pltpu.VMEM((2 * tokens, features), jnp.bfloat16),
            pltpu.VMEM((count_f, features, block), jnp.bfloat16),
            pltpu.VMEM((count_f, 2 * rank + 2 * channels, block), jnp.bfloat16),
            pltpu.VMEM((2 * tokens, width), jnp.bfloat16),
            pltpu.VMEM((count_f, 2 * tokens, block), jnp.float32),
            pltpu.VMEM((count_f, tokens, block), jnp.bfloat16),
            pltpu.VMEM((count_f, tokens, block), jnp.float32),
            pltpu.VMEM((count_f, tokens, block), jnp.bfloat16),
            pltpu.SemaphoreType.DMA((6 + 2 * len(chunks),)),
        ],
        compiler_params=pltpu.CompilerParams(vmem_limit_bytes=60 * 1024 * 1024),
        name="step",
    )(where, *operands, *chunks)


def gather_chunks(own, own_small, seq_index):
    count_f, count_s = lax.axis_size("fsdp"), lax.axis_size("seq")
    part, small_part = own.shape[0] // count_s, own_small.shape[0] // count_s
    columns = own.shape[1]
    chunk = jnp.concatenate(
        [
            lax.dynamic_slice(own, (seq_index * part, 0), (part, columns)),
            lax.dynamic_slice(own_small, (seq_index * small_part, 0), (small_part, columns)),
        ],
        axis=0,
    )
    chunks = []
    for held in [shift(chunk, step) for step in range(1, count_f)]:
        for mask in range(count_s // 2):
            piece = swap(held, 2 * mask) if mask else held
            chunks += [piece, swap(piece, 1)]
    return chunks


def dense_step(
    fsdp_index,
    seq_index,
    reference_attention,
    policy_attention,
    reference_residual,
    policy_residual,
    noise,
    latent,
    modulation,
    frozen_output_weight,
    small_weights,
    rank,
    scale_total,
):
    feature_index, block = frozen_output_weight.shape
    tokens, layer_width = reference_residual.shape
    channel_count = noise.shape[1]
    count_f = lax.axis_size("fsdp")
    down_block = feature_index // count_f
    gate_row = modulation[:, :layer_width]
    shift_row = modulation[:, layer_width : 2 * layer_width]
    scale_row = modulation[:, 2 * layer_width :]
    ext = jnp.concatenate([frozen_output_weight, small_weights], axis=0)
    full = gather_weights(ext, fsdp_index, seq_index)
    base_full = full[:feature_index]
    up_full = full[feature_index : feature_index + rank]
    head_ref_full = full[feature_index + rank : feature_index + rank + channel_count]
    head_pol_full = full[feature_index + rank + channel_count : feature_index + rank + 2 * channel_count]
    down_full = (
        full[feature_index + rank + 2 * channel_count :]
        .reshape(rank, count_f, block)[:, :, :down_block]
        .reshape(rank, feature_index)
    )

    rows_ref, policy_rows = reference_attention, policy_attention
    stream_ref, stream_pol = reference_residual, policy_residual
    target = noise - latent
    tok_seq = tokens // 2
    sign_rows = jnp.concatenate(
        [jnp.ones((tok_seq, 1), jnp.float32), -jnp.ones((tok_seq, 1), jnp.float32)], axis=0
    )
    proj_ref = jnp.dot(rows_ref, base_full, preferred_element_type=jnp.float32)
    normed_ref, inv_ref, z_ref, pred_ref = final_layer(
        proj_ref, stream_ref, gate_row, shift_row, scale_row, head_ref_full
    )
    part_ref = member_errors(pred_ref, target, scale_total)
    low_rank_rows = contracted_columns(policy_rows, down_full).astype(jnp.bfloat16)
    policy_projection = jnp.dot(
        policy_rows, base_full, preferred_element_type=jnp.float32
    ) + jnp.dot(low_rank_rows, up_full, preferred_element_type=jnp.float32)
    normed_pol, inv_pol, z_pol, pred_pol = final_layer(
        policy_projection, stream_pol, gate_row, shift_row, scale_row, head_pol_full
    )
    part_pol = member_errors(pred_pol, target, scale_total)
    local_margin = part_pol[0] - part_ref[0] - (part_pol[1] - part_ref[1])
    margin_row = jnp.full((8, 128), local_margin, jnp.float32)

    dpred = (sign_rows * 2.0 * (pred_pol - target)).astype(jnp.bfloat16)
    head_part = contract_rows(dpred, z_pol)
    dz_rows = jnp.dot(dpred, head_pol_full, preferred_element_type=jnp.float32)
    dn_rows = dz_rows * (1.0 + scale_row)
    dstream = inv_pol * (
        dn_rows
        - jnp.mean(dn_rows, axis=1, keepdims=True)
        - normed_pol * jnp.mean(dn_rows * normed_pol, axis=1, keepdims=True)
    )
    projection_gradient = (gate_row * dstream).astype(jnp.bfloat16)
    up_part = contract_rows(low_rank_rows, projection_gradient)
    low_rank_gradient = contracted_columns(projection_gradient, up_full).astype(jnp.bfloat16)
    down_part = contract_rows(low_rank_gradient, policy_rows)
    attn = contracted_columns(projection_gradient, base_full) + jnp.dot(
        low_rank_gradient, down_full, preferred_element_type=jnp.float32
    )

    def blocks(value):
        return value.astype(jnp.bfloat16).reshape(value.shape[0], count_f, -1).transpose(1, 0, 2)

    grads = jnp.concatenate([blocks(down_part), blocks(up_part), blocks(head_part)], axis=2)
    grads = grads.reshape(count_f, 2, rank // 2, -1)
    core = seq_index % 2
    return (pick(grads, core, 1), pick(grads, 1 - core, 1), margin_row, dstream, attn)


def local(
    timestep,
    pooled,
    modulation_weight,
    reference_attention,
    policy_attention,
    reference_residual,
    policy_residual,
    noise,
    latent,
    frozen_output_weight,
    adapter_down_weight,
    adapter_up_weight,
    reference_head,
    policy_head,
):
    layer_width = pooled.shape[1]
    feature_index = reference_attention.shape[-1]
    channel_count = noise.shape[-1]
    rank = adapter_down_weight.shape[0]
    tok_seq = reference_attention.shape[2]
    count_f, count_s = lax.axis_size("fsdp"), lax.axis_size("seq")
    fsdp_index, seq_index = lax.axis_index("fsdp"), lax.axis_index("seq")
    length = tok_seq * count_s
    scale_total = float(length * channel_count)
    beta = math.sqrt(length * channel_count) / 8.0

    cond_vec = pooled.astype(jnp.float32) + embedding(timestep, layer_width)
    activated = jax.nn.silu(cond_vec).astype(jnp.bfloat16)
    by_block = activated.reshape(pooled.shape[0], count_f, -1).transpose(1, 0, 2)
    pieces = [pick(by_block, fsdp_index)]
    for step in range(1, count_f):
        pieces.append(shift(pick(by_block, (fsdp_index + step) % count_f), step))
    per_pair = pooled.shape[0]
    partial_value = jnp.dot(
        jnp.concatenate(pieces, axis=0), modulation_weight, preferred_element_type=jnp.float32
    )
    own_part = partial_value[:per_pair]
    for step in range(1, count_f):
        own_part = own_part + shift(
            partial_value[per_pair * step : per_pair * (step + 1)], count_f - step
        )
    modulation = gather_seq(own_part, seq_index).transpose(1, 0, 2).reshape(per_pair, -1)

    block = frozen_output_weight.shape[1]
    down_block = adapter_down_weight.shape[1]
    small_weights = jnp.concatenate(
        [
            adapter_up_weight,
            reference_head,
            policy_head,
            jnp.pad(adapter_down_weight, ((0, 0), (0, block - down_block))),
        ],
        axis=0,
    )
    tokens = 2 * tok_seq
    inputs = (
        policy_attention.reshape(tokens, feature_index),
        reference_attention.reshape(tokens, feature_index),
        policy_residual.reshape(tokens, layer_width),
        reference_residual.reshape(tokens, layer_width),
        noise.reshape(tokens, channel_count),
        latent.reshape(tokens, channel_count),
        modulation,
        frozen_output_weight,
        small_weights,
    )
    part, small_part = feature_index // count_s, small_weights.shape[0] // count_s
    if down_block % 128 or block % 128 or part % 16 or small_part % 16 or rank % 32:
        keep, send, margin_row, dstream, attn = dense_step(
            fsdp_index,
            seq_index,
            inputs[1],
            inputs[0],
            inputs[3],
            inputs[2],
            *inputs[4:],
            rank,
            scale_total,
        )
    else:
        keep, send, margin_row, dstream, attn = step_call(
            jnp.stack([fsdp_index, seq_index]).astype(jnp.int32),
            inputs,
            gather_chunks(frozen_output_weight, small_weights, seq_index),
            tokens,
            feature_index,
            layer_width,
            rank,
            channel_count,
            scale_total,
        )

    plane_count, plane_index = count_s // 2, seq_index // 2
    width = keep.shape[2]
    half = (keep.astype(jnp.float32) + swap(send, 1).astype(jnp.float32)).astype(jnp.bfloat16)
    half = half.reshape(count_f, plane_count, rank // count_s, width)
    total = pick(half, plane_index, 1).astype(jnp.float32)
    for mask in range(1, plane_count):
        total = total + swap(pick(half, plane_index ^ mask, 1), 2 * mask).astype(jnp.float32)
    margin = jnp.sum(gather_seq(margin_row, seq_index)[:, 0, 0])
    loss = jax.nn.softplus(beta * margin).reshape(1)
    weight_pair = jax.nn.sigmoid(beta * margin)
    grad_resid = (weight_pair * dstream).astype(jnp.bfloat16).reshape(policy_residual.shape)
    grad_attn = (weight_pair * attn).astype(jnp.bfloat16).reshape(policy_attention.shape)
    pair_sum = (weight_pair * total).astype(jnp.bfloat16)
    own_sum = pick(pair_sum, fsdp_index).astype(jnp.float32)
    for step in range(1, count_f):
        own_sum = own_sum + shift(pick(pair_sum, (fsdp_index + step) % count_f), step).astype(
            jnp.float32
        )
    gathered = gather_seq(own_sum.astype(jnp.bfloat16), seq_index)
    gathered = gathered.reshape(plane_count, 2, rank // count_s, width).transpose(1, 0, 2, 3)
    sums = gathered.reshape(rank, width).astype(jnp.float32)
    square = jnp.full((8, 128), jnp.sum(sums * sums), jnp.float32)
    total_square = square
    for step in range(1, count_f):
        total_square = total_square + shift(square, step)
    upper_limit = math.sqrt(
        rank * feature_index + rank * layer_width + channel_count * layer_width
    )
    factor = jnp.minimum(1.0, upper_limit / jnp.sqrt(total_square[0, 0] + 1e-12))
    scaled = factor * sums
    return (
        loss,
        scaled[:, :down_block],
        scaled[:, down_block : down_block + block],
        scaled[:, down_block + block :],
        grad_resid,
        grad_attn,
    )


def solution(mesh):
    in_specs = (
        P("fsdp"),
        P("fsdp", None),
        P("fsdp", "seq"),
        P("fsdp", None, "seq", None),
        P("fsdp", None, "seq", None),
        P("fsdp", None, "seq", None),
        P("fsdp", None, "seq", None),
        P("fsdp", None, "seq", None),
        P("fsdp", None, "seq", None),
        P(None, "fsdp"),
        P(None, "fsdp"),
        P(None, "fsdp"),
        P(None, "fsdp"),
        P(None, "fsdp"),
    )
    out_specs = (
        P("fsdp"),
        P(None, "fsdp"),
        P(None, "fsdp"),
        P(None, "fsdp"),
        P("fsdp", None, "seq", None),
        P("fsdp", None, "seq", None),
    )
    return jax.shard_map(local, mesh=mesh, in_specs=in_specs, out_specs=out_specs, check_vma=False)
```

```python
import math

import jax
import jax.numpy as jnp
from jax import lax
from jax.experimental import pallas as pl
from jax.experimental.pallas import tpu as pltpu
from jax.sharding import PartitionSpec as P


EPSILON = 1e-06


def embedding(timestep, layer_width):
    half_width = layer_width // 2
    frequency = jnp.exp(-math.log(10000.0) * jnp.arange(half_width, dtype=jnp.float32) / half_width)
    angles = timestep.astype(jnp.float32)[:, None] * frequency[None, :]
    return jnp.concatenate([jnp.cos(angles), jnp.sin(angles)], axis=1)


def contract_rows(left, right):
    return lax.dot_general(
        left, right, (((0,), (0,)), ((), ())), preferred_element_type=jnp.float32
    )


def contracted_columns(left, right):
    return lax.dot_general(
        left, right, (((1,), (1,)), ((), ())), preferred_element_type=jnp.float32
    )


def shift(value, step):
    count = lax.axis_size("fsdp")
    return lax.ppermute(value, "fsdp", [(i, (i + step) % count) for i in range(count)])


def swap(value, mask):
    count = lax.axis_size("seq")
    return lax.ppermute(value, "seq", [(i, i ^ mask) for i in range(count)])


def pick(value, index, axis=0):
    return lax.dynamic_index_in_dim(value, index, axis, keepdims=False)


def in_order(pieces, index):
    stacked = jnp.stack(pieces)
    places = [pick(stacked, index ^ place) for place in range(len(pieces))]
    return jnp.stack(places)


def gather_seq(value, seq_index):
    count = lax.axis_size("seq")
    plane = [value] + [swap(value, 2 * mask) for mask in range(1, count // 2)]
    stacked = jnp.stack(plane)
    other = swap(stacked, 1)
    both = []
    for mask in range(count // 2):
        both += [stacked[mask], other[mask]]
    return in_order(both, seq_index)


def final_layer(projected, residual, gate_row, shift_row, scale_row, head):
    stream = residual.astype(jnp.float32) + gate_row * projected
    row_mean = jnp.mean(stream, axis=1, keepdims=True)
    centred = stream - row_mean
    variance = jnp.mean(centred * centred, axis=1, keepdims=True)
    inv_std = lax.rsqrt(variance + EPSILON)
    normed = centred * inv_std
    modulated = (normed * (1.0 + scale_row) + shift_row).astype(jnp.bfloat16)
    predicted = contracted_columns(modulated, head)
    return (normed, inv_std, modulated, predicted)


def member_errors(predicted, target, scale_total):
    offset = predicted - target
    squared = jnp.sum(offset * offset, axis=1)
    return jnp.sum(squared.reshape(2, -1), axis=1) / scale_total


def gather_weights(ext, fsdp_index, seq_index):
    rows, columns = ext.shape
    count_f, count_s = lax.axis_size("fsdp"), lax.axis_size("seq")
    part = rows // count_s
    chunk = lax.dynamic_slice(ext, (seq_index * part, 0), (part, columns))
    full = jnp.zeros((rows, columns * count_f), ext.dtype)
    full = lax.dynamic_update_slice(full, ext, (0, fsdp_index * columns))
    arrived = [shift(chunk, step) for step in range(1, count_f)]
    group = -(-len(arrived) // 3)
    for first in range(1, count_f, group):
        steps = range(first, min(first + group, count_f))
        own = jnp.concatenate([arrived[step - 1] for step in steps], axis=0)
        plane = [own] + [swap(own, 2 * mask) for mask in range(1, count_s // 2)]
        pieces = []
        for piece in plane:
            pieces += [piece, swap(piece, 1)]

        def place(at, full, piece, mask):
            row = (seq_index ^ mask) * part
            column = ((fsdp_index - first - at) % count_f) * columns
            held = lax.dynamic_slice(piece, (at * part, 0), (part, columns))
            return lax.dynamic_update_slice(full, held, (row, column))

        for mask, piece in enumerate(pieces):
            if group == 1:
                full = place(0, full, piece, mask)
            else:
                full = lax.fori_loop(
                    0, len(steps), lambda at, held: place(at, held, piece, mask), full
                )
    return full


def dot(left, right):
    return jnp.dot(left, right, preferred_element_type=jnp.float32)


def margin_lanes(filled, seq_index, rounded):
    lane = lax.broadcasted_iota(jnp.int32, filled.shape, 1) - 3 * seq_index
    high = rounded(filled)
    middle = rounded(filled - high)
    low = filled - high - middle
    return jnp.where(
        lane == 0, high, jnp.where(lane == 1, middle, jnp.where(lane == 2, low, 0.0))
    )


def step_kernel(sizes, where, *refs):
    tokens, features, width, rank, channels, count_f, count_s, scale_total, spans = sizes
    block, down_block = width // count_f, features // count_f
    part, small_part = features // count_s, (2 * rank + 2 * channels) // count_s
    (attn_pol, attn_ref, res_pol, res_ref, noise, latent, own, own_small), refs = refs[:8], refs[8:]
    mod_pieces, refs = refs[:count_s], refs[count_s:]
    chunks, refs = refs[: len(spans)], refs[len(spans) :]
    keep, send, dstream_out, attn_out, refs = *refs[:4], refs[4:]
    rows, base, small, residual, proj, z_hold, back, dproj, mod_hold, mod, sems = refs
    fsdp_index, seq_index = where[0], where[1]

    def start(source, target, slot):
        copy = pltpu.make_async_copy(source, target, sems.at[slot])
        copy.start()
        return copy

    first = [
        start(attn_pol, rows.at[:tokens], 0),
        start(attn_ref, rows.at[tokens:], 1),
    ]
    blocks = [[start(own, base.at[fsdp_index], 2)]] + [[] for _ in range(1, count_f)]
    smalls = [start(own_small, small.at[fsdp_index], 3)]
    slot = 6
    for chunk, (step, mask, first_row, count) in zip(chunks, spans):
        at = lax.rem(fsdp_index - step + count_f, count_f)
        place = lax.bitwise_xor(seq_index, mask)
        wide = max(0, min(part - first_row, count))
        if wide:
            row = pl.multiple_of(place * part + first_row, 16)
            blocks[step].append(
                start(chunk.at[:wide], base.at[at, pl.ds(row, wide)], slot)
            )
        if wide < count:
            row = pl.multiple_of(place * small_part + (first_row + wide - part), 16)
            smalls.append(
                start(chunk.at[wide:], small.at[at, pl.ds(row, count - wide)], slot + 1)
            )
        slot += 2
    late = [
        start(res_pol, residual.at[:tokens], 4),
        start(res_ref, residual.at[tokens:], 5),
    ]
    for mask in range(count_s):
        place = lax.bitwise_xor(seq_index, mask)
        late.append(start(mod_pieces[mask], mod_hold.at[place], slot + mask))
    for copy in first:
        copy.wait()
    for step in range(count_f):
        for copy in blocks[step]:
            copy.wait()
        at = lax.rem(fsdp_index - step + count_f, count_f)
        proj[at] = dot(rows[...], base[at])
    for copy in smalls + late:
        copy.wait()
    mod_part = mod_hold.shape[2]
    for place in range(count_s):
        mod[:, place * mod_part : (place + 1) * mod_part] = mod_hold[place]

    def up_of(g):
        return small[g, :rank]

    def head_of(g, policy):
        first_row = rank + (channels if policy else 0)
        return small[g, first_row : first_row + channels]

    def down_of(g):
        return small[g, rank + 2 * channels :, :down_block]

    def columns(g):
        return slice(g * block, (g + 1) * block)

    def gate_of(g):
        return mod[:, g * block : (g + 1) * block]

    def shift_of(g):
        return mod[:, width + g * block : width + (g + 1) * block]

    def scale_of(g):
        return 1.0 + mod[:, 2 * width + g * block : 2 * width + (g + 1) * block]

    low = jnp.zeros((tokens, rank), jnp.float32)
    for g in range(count_f):
        low = low + contracted_columns(
            rows[:tokens, g * down_block : (g + 1) * down_block], down_of(g)
        )
    low_rows = low.astype(jnp.bfloat16)
    row_sum = jnp.zeros((2 * tokens, 1), jnp.float32)
    for g in range(count_f):
        proj[g, :tokens] = proj[g, :tokens] + dot(low_rows, up_of(g))
        stream = residual[:, columns(g)].astype(jnp.float32) + gate_of(g) * proj[g]
        proj[g] = stream
        row_sum = row_sum + jnp.sum(stream, axis=1, keepdims=True)
    mean = row_sum / width
    square_sum = jnp.zeros((2 * tokens, 1), jnp.float32)
    for g in range(count_f):
        centred = proj[g] - mean
        square_sum = square_sum + jnp.sum(centred * centred, axis=1, keepdims=True)
    inv_std = lax.rsqrt(square_sum / width + EPSILON)
    pred_pol = jnp.zeros((tokens, channels), jnp.float32)
    pred_ref = jnp.zeros((tokens, channels), jnp.float32)
    for g in range(count_f):
        normed = (proj[g] - mean) * inv_std
        proj[g] = normed
        z_rows = (normed * scale_of(g) + shift_of(g)).astype(jnp.bfloat16)
        z_hold[g] = z_rows[:tokens]
        pred_pol = pred_pol + contracted_columns(z_rows[:tokens], head_of(g, True))
        pred_ref = pred_ref + contracted_columns(z_rows[tokens:], head_of(g, False))
    target = noise[...] - latent[...]
    half_rows = lax.broadcasted_iota(jnp.int32, (tokens, channels), 0) < tokens // 2
    sign = jnp.where(half_rows, 1.0, -1.0)
    off_pol, off_ref = pred_pol - target, pred_ref - target
    local_margin = jnp.sum(sign * (off_pol * off_pol - off_ref * off_ref)) / scale_total
    lanes = margin_lanes(
        jnp.full((rank // 2, 128), local_margin, jnp.float32),
        seq_index,
        lambda value: value.astype(jnp.bfloat16).astype(jnp.float32),
    ).astype(jnp.bfloat16)
    for g in range(count_f):
        keep[g, :, down_block + 2 * block :] = lanes
        send[g, :, down_block + 2 * block :] = lanes
    dpred_wide = 2.0 * sign * off_pol
    dpred = dpred_wide.astype(jnp.bfloat16)
    dpred_turned = dpred_wide.T.astype(jnp.bfloat16)
    low_turned = low.T.astype(jnp.bfloat16)
    sum_dn = jnp.zeros((tokens, 1), jnp.float32)
    sum_dn_normed = jnp.zeros((tokens, 1), jnp.float32)
    half = rank // 2
    core = lax.rem(seq_index, 2)

    def put(g, first_column, value):
        value = value.astype(jnp.bfloat16).astype(jnp.float32)
        last_column = first_column + value.shape[1]
        top, bottom = value[:half], value[half:]
        keep[g, :, first_column:last_column] = jnp.where(core == 0, top, bottom).astype(jnp.bfloat16)
        send[g, :, first_column:last_column] = jnp.where(core == 0, bottom, top).astype(jnp.bfloat16)

    for g in range(count_f):
        put(g, down_block + block, dot(dpred_turned, z_hold[g]))
        dn_rows = dot(dpred, head_of(g, True)) * scale_of(g)
        back[g] = dn_rows
        sum_dn = sum_dn + jnp.sum(dn_rows, axis=1, keepdims=True)
        sum_dn_normed = sum_dn_normed + jnp.sum(dn_rows * proj[g, :tokens], axis=1, keepdims=True)
    mean_dn, mean_dn_normed = sum_dn / width, sum_dn_normed / width
    inv_pol = inv_std[:tokens]
    low_grad = jnp.zeros((tokens, rank), jnp.float32)
    for g in range(count_f):
        dstream = inv_pol * (back[g] - mean_dn - proj[g, :tokens] * mean_dn_normed)
        dstream_out[:, columns(g)] = dstream
        dproj_rows = (gate_of(g) * dstream).astype(jnp.bfloat16)
        dproj[g] = dproj_rows
        put(g, down_block, dot(low_turned, dproj_rows))
        low_grad = low_grad + contracted_columns(dproj_rows, up_of(g))
    low_grad_rows = low_grad.astype(jnp.bfloat16)
    low_grad_turned = low_grad.T.astype(jnp.bfloat16)
    for g in range(count_f):
        put(g, 0, dot(low_grad_turned, rows[:tokens, g * down_block : (g + 1) * down_block]))
    for g in range(count_f):
        at = slice(g * down_block, (g + 1) * down_block)
        value = dot(low_grad_rows, down_of(g))
        for other in range(count_f):
            value = value + contracted_columns(dproj[other], base[other, at])
        attn_out[:, at] = value


def step_call(where, operands, chunks, spans, tokens, features, width, rank, channels, scale_total):
    count_f, count_s = lax.axis_size("fsdp"), lax.axis_size("seq")
    sizes = (tokens, features, width, rank, channels, count_f, count_s, scale_total, spans)
    block = width // count_f
    grads = jax.ShapeDtypeStruct(
        (count_f, rank // 2, features // count_f + 2 * block + 128), jnp.bfloat16
    )
    any_space = pl.BlockSpec(memory_space=pl.ANY)
    vmem = pl.BlockSpec(memory_space=pltpu.VMEM)
    return pl.pallas_call(
        lambda *refs: step_kernel(sizes, *refs),
        out_shape=(
            grads,
            grads,
            jax.ShapeDtypeStruct((tokens, width), jnp.float32),
            jax.ShapeDtypeStruct((tokens, features), jnp.float32),
        ),
        in_specs=[pl.BlockSpec(memory_space=pltpu.SMEM)]
        + [any_space] * 4
        + [vmem] * 2
        + [any_space] * (len(operands) - 6 + len(chunks)),
        out_specs=(vmem,) * 4,
        scratch_shapes=[
            pltpu.VMEM((2 * tokens, features), jnp.bfloat16),
            pltpu.VMEM((count_f, features, block), jnp.bfloat16),
            pltpu.VMEM((count_f, 2 * rank + 2 * channels, block), jnp.bfloat16),
            pltpu.VMEM((2 * tokens, width), jnp.bfloat16),
            pltpu.VMEM((count_f, 2 * tokens, block), jnp.float32),
            pltpu.VMEM((count_f, tokens, block), jnp.bfloat16),
            pltpu.VMEM((count_f, tokens, block), jnp.float32),
            pltpu.VMEM((count_f, tokens, block), jnp.bfloat16),
            pltpu.VMEM((count_s, 1, 3 * width // count_s), jnp.float32),
            pltpu.VMEM((1, 3 * width), jnp.float32),
            pltpu.SemaphoreType.DMA((6 + 2 * len(chunks) + count_s,)),
        ],
        compiler_params=pltpu.CompilerParams(vmem_limit_bytes=60 * 1024 * 1024),
        name="step",
    )(where, *operands, *chunks)


def gather_chunks(own, own_small, seq_index):
    count_f, count_s = lax.axis_size("fsdp"), lax.axis_size("seq")
    part, small_part = own.shape[0] // count_s, own_small.shape[0] // count_s
    columns = own.shape[1]
    chunk = jnp.concatenate(
        [
            lax.dynamic_slice(own, (seq_index * part, 0), (part, columns)),
            lax.dynamic_slice(own_small, (seq_index * small_part, 0), (small_part, columns)),
        ],
        axis=0,
    )
    arrived = []
    for step in range(1, count_f):
        arrived.append(shift(chunk, step))
    middle = (part + small_part) // 32 * 16
    chunks, spans = [], []

    def add(step, mask, first_row, piece):
        chunks.extend([piece, swap(piece, 1)])
        spans.append((step, mask, first_row, piece.shape[0]))
        spans.append((step, mask + 1, first_row, piece.shape[0]))

    for step in range(1, count_f):
        held = arrived[step - 1]
        add(step, 0, 0, held)
        if count_s == 8:
            first, second = swap(held, 2), swap(held, 4)
            top, bottom = swap(first[:middle], 4), swap(second[middle:], 2)
            add(step, 2, 0, first)
            add(step, 4, 0, second)
            add(step, 6, 0, top)
            add(step, 6, middle, bottom)
        else:
            for mask in range(2, count_s, 2):
                add(step, mask, 0, swap(held, mask))
    return chunks, tuple(spans)


def dense_step(
    fsdp_index,
    seq_index,
    reference_attention,
    policy_attention,
    reference_residual,
    policy_residual,
    noise,
    latent,
    modulation,
    frozen_output_weight,
    small_weights,
    rank,
    scale_total,
):
    feature_index, block = frozen_output_weight.shape
    tokens, layer_width = reference_residual.shape
    channel_count = noise.shape[1]
    count_f = lax.axis_size("fsdp")
    down_block = feature_index // count_f
    gate_row = modulation[:, :layer_width]
    shift_row = modulation[:, layer_width : 2 * layer_width]
    scale_row = modulation[:, 2 * layer_width :]
    ext = jnp.concatenate([frozen_output_weight, small_weights], axis=0)
    full = gather_weights(ext, fsdp_index, seq_index)
    base_full = full[:feature_index]
    up_full = full[feature_index : feature_index + rank]
    head_ref_full = full[feature_index + rank : feature_index + rank + channel_count]
    head_pol_full = full[feature_index + rank + channel_count : feature_index + rank + 2 * channel_count]
    down_full = (
        full[feature_index + rank + 2 * channel_count :]
        .reshape(rank, count_f, block)[:, :, :down_block]
        .reshape(rank, feature_index)
    )

    rows_ref, policy_rows = reference_attention, policy_attention
    stream_ref, stream_pol = reference_residual, policy_residual
    target = noise - latent
    tok_seq = tokens // 2
    sign_rows = jnp.concatenate(
        [jnp.ones((tok_seq, 1), jnp.float32), -jnp.ones((tok_seq, 1), jnp.float32)], axis=0
    )
    proj_ref = jnp.dot(rows_ref, base_full, preferred_element_type=jnp.float32)
    _, _, _, pred_ref = final_layer(
        proj_ref, stream_ref, gate_row, shift_row, scale_row, head_ref_full
    )
    part_ref = member_errors(pred_ref, target, scale_total)
    low_rank_rows = contracted_columns(policy_rows, down_full).astype(jnp.bfloat16)
    policy_projection = jnp.dot(
        policy_rows, base_full, preferred_element_type=jnp.float32
    ) + jnp.dot(low_rank_rows, up_full, preferred_element_type=jnp.float32)
    normed_pol, inv_pol, z_pol, pred_pol = final_layer(
        policy_projection, stream_pol, gate_row, shift_row, scale_row, head_pol_full
    )
    part_pol = member_errors(pred_pol, target, scale_total)
    local_margin = part_pol[0] - part_ref[0] - (part_pol[1] - part_ref[1])
    lanes = margin_lanes(
        jnp.full((rank, 128), local_margin, jnp.float32),
        seq_index,
        lambda value: lax.reduce_precision(value, 8, 7),
    ).astype(jnp.bfloat16)

    dpred = (sign_rows * 2.0 * (pred_pol - target)).astype(jnp.bfloat16)
    head_part = contract_rows(dpred, z_pol)
    dz_rows = jnp.dot(dpred, head_pol_full, preferred_element_type=jnp.float32)
    dn_rows = dz_rows * (1.0 + scale_row)
    dstream = inv_pol * (
        dn_rows
        - jnp.mean(dn_rows, axis=1, keepdims=True)
        - normed_pol * jnp.mean(dn_rows * normed_pol, axis=1, keepdims=True)
    )
    projection_gradient = (gate_row * dstream).astype(jnp.bfloat16)
    up_part = contract_rows(low_rank_rows, projection_gradient)
    low_rank_gradient = contracted_columns(projection_gradient, up_full).astype(jnp.bfloat16)
    down_part = contract_rows(low_rank_gradient, policy_rows)
    attn = contracted_columns(projection_gradient, base_full) + jnp.dot(
        low_rank_gradient, down_full, preferred_element_type=jnp.float32
    )

    def blocks(value):
        return value.astype(jnp.bfloat16).reshape(value.shape[0], count_f, -1).transpose(1, 0, 2)

    lanes = jnp.broadcast_to(lanes[None], (count_f,) + lanes.shape)
    grads = jnp.concatenate([blocks(down_part), blocks(up_part), blocks(head_part), lanes], axis=2)
    grads = grads.reshape(count_f, 2, rank // 2, -1)
    core = seq_index % 2
    return (pick(grads, core, 1), pick(grads, 1 - core, 1), dstream, attn)


def local(
    timestep,
    pooled,
    modulation_weight,
    reference_attention,
    policy_attention,
    reference_residual,
    policy_residual,
    noise,
    latent,
    frozen_output_weight,
    adapter_down_weight,
    adapter_up_weight,
    reference_head,
    policy_head,
):
    layer_width = pooled.shape[1]
    feature_index = reference_attention.shape[-1]
    channel_count = noise.shape[-1]
    rank = adapter_down_weight.shape[0]
    tok_seq = reference_attention.shape[2]
    count_f, count_s = lax.axis_size("fsdp"), lax.axis_size("seq")
    fsdp_index, seq_index = lax.axis_index("fsdp"), lax.axis_index("seq")
    length = tok_seq * count_s
    scale_total = float(length * channel_count)
    beta = math.sqrt(length * channel_count) / 8.0

    cond_vec = pooled.astype(jnp.float32) + embedding(timestep, layer_width)
    activated = jax.nn.silu(cond_vec).astype(jnp.bfloat16)
    by_block = activated.reshape(pooled.shape[0], count_f, -1).transpose(1, 0, 2)
    pieces = [pick(by_block, fsdp_index)]
    for step in range(1, count_f):
        pieces.append(shift(pick(by_block, (fsdp_index + step) % count_f), step))
    per_pair = pooled.shape[0]
    partial_value = jnp.dot(
        jnp.concatenate(pieces, axis=0), modulation_weight, preferred_element_type=jnp.float32
    )
    own_part = partial_value[:per_pair]
    for step in range(1, count_f):
        own_part = own_part + shift(
            partial_value[per_pair * step : per_pair * (step + 1)], count_f - step
        )
    mod_plane = [own_part] + [swap(own_part, 2 * mask) for mask in range(1, count_s // 2)]
    mod_pieces = []
    for piece in mod_plane:
        mod_pieces += [piece, swap(piece, 1)]

    block = frozen_output_weight.shape[1]
    down_block = adapter_down_weight.shape[1]
    small_weights = jnp.concatenate(
        [
            adapter_up_weight,
            reference_head,
            policy_head,
            jnp.pad(adapter_down_weight, ((0, 0), (0, block - down_block))),
        ],
        axis=0,
    )
    tokens = 2 * tok_seq
    inputs = (
        policy_attention.reshape(tokens, feature_index),
        reference_attention.reshape(tokens, feature_index),
        policy_residual.reshape(tokens, layer_width),
        reference_residual.reshape(tokens, layer_width),
        noise.reshape(tokens, channel_count),
        latent.reshape(tokens, channel_count),
        frozen_output_weight,
        small_weights,
        *mod_pieces,
    )
    part, small_part = feature_index // count_s, small_weights.shape[0] // count_s
    if down_block % 128 or block % 128 or part % 16 or small_part % 16 or rank % 32:
        keep, send, dstream, attn = dense_step(
            fsdp_index,
            seq_index,
            inputs[1],
            inputs[0],
            inputs[3],
            inputs[2],
            *inputs[4:6],
            in_order(mod_pieces, seq_index).reshape(1, -1),
            frozen_output_weight,
            small_weights,
            rank,
            scale_total,
        )
    else:
        keep, send, dstream, attn = step_call(
            jnp.stack([fsdp_index, seq_index]).astype(jnp.int32),
            inputs,
            *gather_chunks(frozen_output_weight, small_weights, seq_index),
            tokens,
            feature_index,
            layer_width,
            rank,
            channel_count,
            scale_total,
        )

    plane_count, plane_index = count_s // 2, seq_index // 2
    width = keep.shape[2] - 128
    half = (keep.astype(jnp.float32) + swap(send, 1).astype(jnp.float32)).astype(jnp.bfloat16)
    half = half.reshape(count_f, plane_count, rank // count_s, width + 128)
    total = pick(half, plane_index, 1).astype(jnp.float32)
    for mask in range(1, plane_count):
        total = total + swap(pick(half, plane_index ^ mask, 1), 2 * mask).astype(jnp.float32)
    margin = jnp.sum(total[0, 0, width:])
    loss = jax.nn.softplus(beta * margin).reshape(1)
    weight_pair = jax.nn.sigmoid(beta * margin)
    grad_resid = (weight_pair * dstream).astype(jnp.bfloat16).reshape(policy_residual.shape)
    grad_attn = (weight_pair * attn).astype(jnp.bfloat16).reshape(policy_attention.shape)
    pair_sum = (weight_pair * total[:, :, :width]).astype(jnp.bfloat16)
    own_sum = pick(pair_sum, fsdp_index).astype(jnp.float32)
    for step in range(1, count_f):
        own_sum = own_sum + shift(pick(pair_sum, (fsdp_index + step) % count_f), step).astype(
            jnp.float32
        )
    gathered = gather_seq(own_sum.astype(jnp.bfloat16), seq_index)
    gathered = gathered.reshape(plane_count, 2, rank // count_s, width).transpose(1, 0, 2, 3)
    sums = gathered.reshape(rank, width).astype(jnp.float32)
    square = jnp.full((8, 128), jnp.sum(sums * sums), jnp.float32)
    total_square = square
    for step in range(1, count_f):
        total_square = total_square + shift(square, step)
    upper_limit = math.sqrt(
        rank * feature_index + rank * layer_width + channel_count * layer_width
    )
    factor = jnp.minimum(1.0, upper_limit / jnp.sqrt(total_square[0, 0] + 1e-12))
    scaled = factor * sums
    return (
        loss,
        scaled[:, :down_block],
        scaled[:, down_block : down_block + block],
        scaled[:, down_block + block :],
        grad_resid,
        grad_attn,
    )


def solution(mesh):
    in_specs = (
        P("fsdp"),
        P("fsdp", None),
        P("fsdp", "seq"),
        P("fsdp", None, "seq", None),
        P("fsdp", None, "seq", None),
        P("fsdp", None, "seq", None),
        P("fsdp", None, "seq", None),
        P("fsdp", None, "seq", None),
        P("fsdp", None, "seq", None),
        P(None, "fsdp"),
        P(None, "fsdp"),
        P(None, "fsdp"),
        P(None, "fsdp"),
        P(None, "fsdp"),
    )
    out_specs = (
        P("fsdp"),
        P(None, "fsdp"),
        P(None, "fsdp"),
        P(None, "fsdp"),
        P("fsdp", None, "seq", None),
        P("fsdp", None, "seq", None),
    )

    return jax.shard_map(local, mesh=mesh, in_specs=in_specs, out_specs=out_specs, check_vma=False)
```

```python
import math

import jax
import jax.numpy as jnp
from jax import lax
from jax.experimental import pallas as pl
from jax.experimental.pallas import tpu as pltpu
from jax.sharding import PartitionSpec as P


EPSILON = 1e-06


def embedding(timestep, layer_width):
    half_width = layer_width // 2
    frequency = jnp.exp(-math.log(10000.0) * jnp.arange(half_width, dtype=jnp.float32) / half_width)
    angles = timestep.astype(jnp.float32)[:, None] * frequency[None, :]
    return jnp.concatenate([jnp.cos(angles), jnp.sin(angles)], axis=1)


def contract_rows(left, right):
    return lax.dot_general(
        left, right, (((0,), (0,)), ((), ())), preferred_element_type=jnp.float32
    )


def contracted_columns(left, right):
    return lax.dot_general(
        left, right, (((1,), (1,)), ((), ())), preferred_element_type=jnp.float32
    )


def shift(value, step):
    count = lax.axis_size("fsdp")
    return lax.ppermute(value, "fsdp", [(i, (i + step) % count) for i in range(count)])


def swap(value, mask):
    count = lax.axis_size("seq")
    return lax.ppermute(value, "seq", [(i, i ^ mask) for i in range(count)])


def pick(value, index, axis=0):
    return lax.dynamic_index_in_dim(value, index, axis, keepdims=False)


def in_order(pieces, index):
    stacked = jnp.stack(pieces)
    places = [pick(stacked, index ^ place) for place in range(len(pieces))]
    return jnp.stack(places)


def gather_seq(value, seq_index):
    count = lax.axis_size("seq")
    plane = [value] + [swap(value, 2 * mask) for mask in range(1, count // 2)]
    stacked = jnp.stack(plane)
    other = swap(stacked, 1)
    both = []
    for mask in range(count // 2):
        both += [stacked[mask], other[mask]]
    return in_order(both, seq_index)


def final_layer(projected, residual, gate_row, shift_row, scale_row, head):
    stream = residual.astype(jnp.float32) + gate_row * projected
    row_mean = jnp.mean(stream, axis=1, keepdims=True)
    centred = stream - row_mean
    variance = jnp.mean(centred * centred, axis=1, keepdims=True)
    inv_std = lax.rsqrt(variance + EPSILON)
    normed = centred * inv_std
    modulated = (normed * (1.0 + scale_row) + shift_row).astype(jnp.bfloat16)
    predicted = contracted_columns(modulated, head)
    return (normed, inv_std, modulated, predicted)


def member_errors(predicted, target, scale_total):
    offset = predicted - target
    squared = jnp.sum(offset * offset, axis=1)
    return jnp.sum(squared.reshape(2, -1), axis=1) / scale_total


def gather_weights(ext, fsdp_index, seq_index):
    rows, columns = ext.shape
    count_f, count_s = lax.axis_size("fsdp"), lax.axis_size("seq")
    part = rows // count_s
    chunk = lax.dynamic_slice(ext, (seq_index * part, 0), (part, columns))
    full = jnp.zeros((rows, columns * count_f), ext.dtype)
    full = lax.dynamic_update_slice(full, ext, (0, fsdp_index * columns))
    arrived = [shift(chunk, step) for step in range(1, count_f)]
    group = -(-len(arrived) // 3)
    for first in range(1, count_f, group):
        steps = range(first, min(first + group, count_f))
        own = jnp.concatenate([arrived[step - 1] for step in steps], axis=0)
        plane = [own] + [swap(own, 2 * mask) for mask in range(1, count_s // 2)]
        pieces = []
        for piece in plane:
            pieces += [piece, swap(piece, 1)]

        def place(at, full, piece, mask):
            row = (seq_index ^ mask) * part
            column = ((fsdp_index - first - at) % count_f) * columns
            held = lax.dynamic_slice(piece, (at * part, 0), (part, columns))
            return lax.dynamic_update_slice(full, held, (row, column))

        for mask, piece in enumerate(pieces):
            if group == 1:
                full = place(0, full, piece, mask)
            else:
                full = lax.fori_loop(
                    0, len(steps), lambda at, held: place(at, held, piece, mask), full
                )
    return full


def dot(left, right):
    return jnp.dot(left, right, preferred_element_type=jnp.float32)


def margin_lanes(filled, seq_index, rounded):
    lane = lax.broadcasted_iota(jnp.int32, filled.shape, 1) - 3 * seq_index
    high = rounded(filled)
    middle = rounded(filled - high)
    low = filled - high - middle
    return jnp.where(
        lane == 0, high, jnp.where(lane == 1, middle, jnp.where(lane == 2, low, 0.0))
    )


def step_kernel(sizes, *refs):
    tokens, features, width, rank, channels, count_f, count_s, scale_total, spans = sizes
    block, down_block = width // count_f, features // count_f
    part, small_part = features // count_s, (2 * rank + 2 * channels) // count_s
    (attn_pol, attn_ref, res_pol, res_ref, noise, latent, own, own_small), refs = refs[:8], refs[8:]
    mod_pieces, refs = refs[:count_s], refs[count_s:]
    chunks, refs = refs[: len(spans)], refs[len(spans) :]
    keep, send, dstream_out, attn_out, refs = *refs[:4], refs[4:]
    rows, base, small, residual, proj, z_hold, back, dproj, mod_hold, mod, sems = refs
    fsdp_index, seq_index = lax.axis_index("fsdp"), lax.axis_index("seq")

    def start(source, target, slot):
        copy = pltpu.make_async_copy(source, target, sems.at[slot])
        copy.start()
        return copy

    first = [
        start(attn_pol, rows.at[:tokens], 0),
        start(attn_ref, rows.at[tokens:], 1),
    ]
    blocks = [[start(own, base.at[fsdp_index], 2)]] + [[] for _ in range(1, count_f)]
    smalls = [start(own_small, small.at[fsdp_index], 3)]
    slot = 6
    for chunk, (step, mask, first_row, count) in zip(chunks, spans):
        at = lax.rem(fsdp_index - step + count_f, count_f)
        place = lax.bitwise_xor(seq_index, mask)
        wide = max(0, min(part - first_row, count))
        if wide:
            row = pl.multiple_of(place * part + first_row, 16)
            blocks[step].append(
                start(chunk.at[:wide], base.at[at, pl.ds(row, wide)], slot)
            )
        if wide < count:
            row = pl.multiple_of(place * small_part + (first_row + wide - part), 16)
            smalls.append(
                start(chunk.at[wide:], small.at[at, pl.ds(row, count - wide)], slot + 1)
            )
        slot += 2
    late = [
        start(res_pol, residual.at[:tokens], 4),
        start(res_ref, residual.at[tokens:], 5),
    ]
    for mask in range(count_s):
        place = lax.bitwise_xor(seq_index, mask)
        late.append(start(mod_pieces[mask], mod_hold.at[place], slot + mask))
    for copy in first:
        copy.wait()
    for step in range(count_f):
        for copy in blocks[step]:
            copy.wait()
        at = lax.rem(fsdp_index - step + count_f, count_f)
        proj[at] = dot(rows[...], base[at])
    for copy in smalls + late:
        copy.wait()
    mod_part = mod_hold.shape[2]
    for place in range(count_s):
        mod[:, place * mod_part : (place + 1) * mod_part] = mod_hold[place]

    def up_of(g):
        return small[g, :rank]

    def head_of(g, policy):
        first_row = rank + (channels if policy else 0)
        return small[g, first_row : first_row + channels]

    def down_of(g):
        return small[g, rank + 2 * channels :, :down_block]

    def columns(g):
        return slice(g * block, (g + 1) * block)

    def gate_of(g):
        return mod[:, g * block : (g + 1) * block]

    def shift_of(g):
        return mod[:, width + g * block : width + (g + 1) * block]

    def scale_of(g):
        return 1.0 + mod[:, 2 * width + g * block : 2 * width + (g + 1) * block]

    low = jnp.zeros((tokens, rank), jnp.float32)
    for g in range(count_f):
        low = low + contracted_columns(
            rows[:tokens, g * down_block : (g + 1) * down_block], down_of(g)
        )
    low_rows = low.astype(jnp.bfloat16)
    row_sum = jnp.zeros((2 * tokens, 1), jnp.float32)
    for g in range(count_f):
        proj[g, :tokens] = proj[g, :tokens] + dot(low_rows, up_of(g))
        stream = residual[:, columns(g)].astype(jnp.float32) + gate_of(g) * proj[g]
        proj[g] = stream
        row_sum = row_sum + jnp.sum(stream, axis=1, keepdims=True)
    mean = row_sum / width
    square_sum = jnp.zeros((2 * tokens, 1), jnp.float32)
    for g in range(count_f):
        centred = proj[g] - mean
        square_sum = square_sum + jnp.sum(centred * centred, axis=1, keepdims=True)
    inv_std = lax.rsqrt(square_sum / width + EPSILON)
    pred_pol = jnp.zeros((tokens, channels), jnp.float32)
    pred_ref = jnp.zeros((tokens, channels), jnp.float32)
    for g in range(count_f):
        normed = (proj[g] - mean) * inv_std
        proj[g] = normed
        z_rows = (normed * scale_of(g) + shift_of(g)).astype(jnp.bfloat16)
        z_hold[g] = z_rows[:tokens]
        pred_pol = pred_pol + contracted_columns(z_rows[:tokens], head_of(g, True))
        pred_ref = pred_ref + contracted_columns(z_rows[tokens:], head_of(g, False))
    target = noise[...] - latent[...]
    half_rows = lax.broadcasted_iota(jnp.int32, (tokens, channels), 0) < tokens // 2
    sign = jnp.where(half_rows, 1.0, -1.0)
    off_pol, off_ref = pred_pol - target, pred_ref - target
    local_margin = jnp.sum(sign * (off_pol * off_pol - off_ref * off_ref)) / scale_total
    lanes = margin_lanes(
        jnp.full((rank // 2, 128), local_margin, jnp.float32),
        seq_index,
        lambda value: value.astype(jnp.bfloat16).astype(jnp.float32),
    ).astype(jnp.bfloat16)
    for g in range(count_f):
        keep[g, :, down_block + 2 * block :] = lanes
        send[g, :, down_block + 2 * block :] = lanes
    dpred_wide = 2.0 * sign * off_pol
    dpred = dpred_wide.astype(jnp.bfloat16)
    dpred_turned = dpred_wide.T.astype(jnp.bfloat16)
    low_turned = low.T.astype(jnp.bfloat16)
    sum_dn = jnp.zeros((tokens, 1), jnp.float32)
    sum_dn_normed = jnp.zeros((tokens, 1), jnp.float32)
    half = rank // 2
    core = lax.rem(seq_index, 2)

    def put(g, first_column, value):
        value = value.astype(jnp.bfloat16).astype(jnp.float32)
        last_column = first_column + value.shape[1]
        top, bottom = value[:half], value[half:]
        keep[g, :, first_column:last_column] = jnp.where(core == 0, top, bottom).astype(jnp.bfloat16)
        send[g, :, first_column:last_column] = jnp.where(core == 0, bottom, top).astype(jnp.bfloat16)

    for g in range(count_f):
        put(g, down_block + block, dot(dpred_turned, z_hold[g]))
        dn_rows = dot(dpred, head_of(g, True)) * scale_of(g)
        back[g] = dn_rows
        sum_dn = sum_dn + jnp.sum(dn_rows, axis=1, keepdims=True)
        sum_dn_normed = sum_dn_normed + jnp.sum(dn_rows * proj[g, :tokens], axis=1, keepdims=True)
    mean_dn, mean_dn_normed = sum_dn / width, sum_dn_normed / width
    inv_pol = inv_std[:tokens]
    low_grad = jnp.zeros((tokens, rank), jnp.float32)
    for g in range(count_f):
        dstream = inv_pol * (back[g] - mean_dn - proj[g, :tokens] * mean_dn_normed)
        dstream_out[:, columns(g)] = dstream
        dproj_rows = (gate_of(g) * dstream).astype(jnp.bfloat16)
        dproj[g] = dproj_rows
        put(g, down_block, dot(low_turned, dproj_rows))
        low_grad = low_grad + contracted_columns(dproj_rows, up_of(g))
    low_grad_rows = low_grad.astype(jnp.bfloat16)
    low_grad_turned = low_grad.T.astype(jnp.bfloat16)
    for g in range(count_f):
        put(g, 0, dot(low_grad_turned, rows[:tokens, g * down_block : (g + 1) * down_block]))
    for g in range(count_f):
        at = slice(g * down_block, (g + 1) * down_block)
        value = dot(low_grad_rows, down_of(g))
        for other in range(count_f):
            value = value + contracted_columns(dproj[other], base[other, at])
        attn_out[:, at] = value


def step_call(operands, chunks, spans, tokens, features, width, rank, channels, scale_total):
    count_f, count_s = lax.axis_size("fsdp"), lax.axis_size("seq")
    sizes = (tokens, features, width, rank, channels, count_f, count_s, scale_total, spans)
    block = width // count_f
    grads = jax.ShapeDtypeStruct(
        (count_f, rank // 2, features // count_f + 2 * block + 128), jnp.bfloat16
    )
    any_space = pl.BlockSpec(memory_space=pl.ANY)
    vmem = pl.BlockSpec(memory_space=pltpu.VMEM)
    return pl.pallas_call(
        lambda *refs: step_kernel(sizes, *refs),
        out_shape=(
            grads,
            grads,
            jax.ShapeDtypeStruct((tokens, width), jnp.float32),
            jax.ShapeDtypeStruct((tokens, features), jnp.float32),
        ),
        in_specs=[any_space] * 4
        + [vmem] * 2
        + [any_space] * (len(operands) - 6 + len(chunks)),
        out_specs=(vmem,) * 4,
        scratch_shapes=[
            pltpu.VMEM((2 * tokens, features), jnp.bfloat16),
            pltpu.VMEM((count_f, features, block), jnp.bfloat16),
            pltpu.VMEM((count_f, 2 * rank + 2 * channels, block), jnp.bfloat16),
            pltpu.VMEM((2 * tokens, width), jnp.bfloat16),
            pltpu.VMEM((count_f, 2 * tokens, block), jnp.float32),
            pltpu.VMEM((count_f, tokens, block), jnp.bfloat16),
            pltpu.VMEM((count_f, tokens, block), jnp.float32),
            pltpu.VMEM((count_f, tokens, block), jnp.bfloat16),
            pltpu.VMEM((count_s, 1, 3 * width // count_s), jnp.float32),
            pltpu.VMEM((1, 3 * width), jnp.float32),
            pltpu.SemaphoreType.DMA((6 + 2 * len(chunks) + count_s,)),
        ],
        compiler_params=pltpu.CompilerParams(vmem_limit_bytes=60 * 1024 * 1024),
        name="step",
    )(*operands, *chunks)


def send_chunks(own, own_small, seq_index):
    count_f, count_s = lax.axis_size("fsdp"), lax.axis_size("seq")
    part, small_part = own.shape[0] // count_s, own_small.shape[0] // count_s
    columns = own.shape[1]
    chunk = jnp.concatenate(
        [
            lax.dynamic_slice(own, (seq_index * part, 0), (part, columns)),
            lax.dynamic_slice(own_small, (seq_index * small_part, 0), (small_part, columns)),
        ],
        axis=0,
    )
    arrived = []
    for step in range(1, count_f):
        arrived.append(shift(chunk, step))
    return arrived


def spread_chunks(arrived, part, small_part):
    count_f, count_s = lax.axis_size("fsdp"), lax.axis_size("seq")
    middle = (part + small_part) // 32 * 16
    chunks, spans = [], []

    def add(step, mask, first_row, piece):
        chunks.extend([piece, swap(piece, 1)])
        spans.append((step, mask, first_row, piece.shape[0]))
        spans.append((step, mask + 1, first_row, piece.shape[0]))

    for step in range(1, count_f):
        held = arrived[step - 1]
        add(step, 0, 0, held)
        if count_s == 8:
            first, second = swap(held, 2), swap(held, 4)
            top, bottom = swap(first[:middle], 4), swap(second[middle:], 2)
            add(step, 2, 0, first)
            add(step, 4, 0, second)
            add(step, 6, 0, top)
            add(step, 6, middle, bottom)
        else:
            for mask in range(2, count_s, 2):
                add(step, mask, 0, swap(held, mask))
    return chunks, tuple(spans)


def dense_step(
    fsdp_index,
    seq_index,
    reference_attention,
    policy_attention,
    reference_residual,
    policy_residual,
    noise,
    latent,
    modulation,
    frozen_output_weight,
    small_weights,
    rank,
    scale_total,
):
    feature_index, block = frozen_output_weight.shape
    tokens, layer_width = reference_residual.shape
    channel_count = noise.shape[1]
    count_f = lax.axis_size("fsdp")
    down_block = feature_index // count_f
    gate_row = modulation[:, :layer_width]
    shift_row = modulation[:, layer_width : 2 * layer_width]
    scale_row = modulation[:, 2 * layer_width :]
    ext = jnp.concatenate([frozen_output_weight, small_weights], axis=0)
    full = gather_weights(ext, fsdp_index, seq_index)
    base_full = full[:feature_index]
    up_full = full[feature_index : feature_index + rank]
    head_ref_full = full[feature_index + rank : feature_index + rank + channel_count]
    head_pol_full = full[feature_index + rank + channel_count : feature_index + rank + 2 * channel_count]
    down_full = (
        full[feature_index + rank + 2 * channel_count :]
        .reshape(rank, count_f, block)[:, :, :down_block]
        .reshape(rank, feature_index)
    )

    rows_ref, policy_rows = reference_attention, policy_attention
    stream_ref, stream_pol = reference_residual, policy_residual
    target = noise - latent
    tok_seq = tokens // 2
    sign_rows = jnp.concatenate(
        [jnp.ones((tok_seq, 1), jnp.float32), -jnp.ones((tok_seq, 1), jnp.float32)], axis=0
    )
    proj_ref = jnp.dot(rows_ref, base_full, preferred_element_type=jnp.float32)
    _, _, _, pred_ref = final_layer(
        proj_ref, stream_ref, gate_row, shift_row, scale_row, head_ref_full
    )
    part_ref = member_errors(pred_ref, target, scale_total)
    low_rank_rows = contracted_columns(policy_rows, down_full).astype(jnp.bfloat16)
    policy_projection = jnp.dot(
        policy_rows, base_full, preferred_element_type=jnp.float32
    ) + jnp.dot(low_rank_rows, up_full, preferred_element_type=jnp.float32)
    normed_pol, inv_pol, z_pol, pred_pol = final_layer(
        policy_projection, stream_pol, gate_row, shift_row, scale_row, head_pol_full
    )
    part_pol = member_errors(pred_pol, target, scale_total)
    local_margin = part_pol[0] - part_ref[0] - (part_pol[1] - part_ref[1])
    lanes = margin_lanes(
        jnp.full((rank, 128), local_margin, jnp.float32),
        seq_index,
        lambda value: lax.reduce_precision(value, 8, 7),
    ).astype(jnp.bfloat16)

    dpred = (sign_rows * 2.0 * (pred_pol - target)).astype(jnp.bfloat16)
    head_part = contract_rows(dpred, z_pol)
    dz_rows = jnp.dot(dpred, head_pol_full, preferred_element_type=jnp.float32)
    dn_rows = dz_rows * (1.0 + scale_row)
    dstream = inv_pol * (
        dn_rows
        - jnp.mean(dn_rows, axis=1, keepdims=True)
        - normed_pol * jnp.mean(dn_rows * normed_pol, axis=1, keepdims=True)
    )
    projection_gradient = (gate_row * dstream).astype(jnp.bfloat16)
    up_part = contract_rows(low_rank_rows, projection_gradient)
    low_rank_gradient = contracted_columns(projection_gradient, up_full).astype(jnp.bfloat16)
    down_part = contract_rows(low_rank_gradient, policy_rows)
    attn = contracted_columns(projection_gradient, base_full) + jnp.dot(
        low_rank_gradient, down_full, preferred_element_type=jnp.float32
    )

    def blocks(value):
        return value.astype(jnp.bfloat16).reshape(value.shape[0], count_f, -1).transpose(1, 0, 2)

    lanes = jnp.broadcast_to(lanes[None], (count_f,) + lanes.shape)
    grads = jnp.concatenate([blocks(down_part), blocks(up_part), blocks(head_part), lanes], axis=2)
    grads = grads.reshape(count_f, 2, rank // 2, -1)
    core = seq_index % 2
    return (pick(grads, core, 1), pick(grads, 1 - core, 1), dstream, attn)


def local(
    timestep,
    pooled,
    modulation_weight,
    reference_attention,
    policy_attention,
    reference_residual,
    policy_residual,
    noise,
    latent,
    frozen_output_weight,
    adapter_down_weight,
    adapter_up_weight,
    reference_head,
    policy_head,
):
    layer_width = pooled.shape[1]
    feature_index = reference_attention.shape[-1]
    channel_count = noise.shape[-1]
    rank = adapter_down_weight.shape[0]
    tok_seq = reference_attention.shape[2]
    count_f, count_s = lax.axis_size("fsdp"), lax.axis_size("seq")
    fsdp_index, seq_index = lax.axis_index("fsdp"), lax.axis_index("seq")
    length = tok_seq * count_s
    scale_total = float(length * channel_count)
    beta = math.sqrt(length * channel_count) / 8.0

    block = frozen_output_weight.shape[1]
    down_block = adapter_down_weight.shape[1]
    small_weights = jnp.concatenate(
        [
            adapter_up_weight,
            reference_head,
            policy_head,
            jnp.pad(adapter_down_weight, ((0, 0), (0, block - down_block))),
        ],
        axis=0,
    )
    part, small_part = feature_index // count_s, small_weights.shape[0] // count_s
    dense = down_block % 128 or block % 128 or part % 16 or small_part % 16 or rank % 32
    if not dense:
        arrived = send_chunks(frozen_output_weight, small_weights, seq_index)
        chunks, spans = spread_chunks(arrived, part, small_part)

    cond_vec = pooled.astype(jnp.float32) + embedding(timestep, layer_width)
    activated = jax.nn.silu(cond_vec).astype(jnp.bfloat16)
    by_block = activated.reshape(pooled.shape[0], count_f, -1).transpose(1, 0, 2)
    pieces = [pick(by_block, fsdp_index)]
    for step in range(1, count_f):
        pieces.append(shift(pick(by_block, (fsdp_index + step) % count_f), step))
    per_pair = pooled.shape[0]
    if not dense:
        late = [at for at, (step, mask, *_) in enumerate(spans) if (step, mask) == (count_f - 2, 2)]
        pieces = lax.optimization_barrier((pieces, chunks[late[0]] if late else arrived[-1]))[0]
    partial_value = jnp.dot(
        jnp.concatenate(pieces, axis=0), modulation_weight, preferred_element_type=jnp.float32
    )
    own_part = partial_value[:per_pair]
    for step in range(1, count_f):
        own_part = own_part + shift(
            partial_value[per_pair * step : per_pair * (step + 1)], count_f - step
        )
    mod_plane = [own_part] + [swap(own_part, 2 * mask) for mask in range(1, count_s // 2)]
    mod_pieces = []
    for piece in mod_plane:
        mod_pieces += [piece, swap(piece, 1)]

    tokens = 2 * tok_seq
    inputs = (
        policy_attention.reshape(tokens, feature_index),
        reference_attention.reshape(tokens, feature_index),
        policy_residual.reshape(tokens, layer_width),
        reference_residual.reshape(tokens, layer_width),
        noise.reshape(tokens, channel_count),
        latent.reshape(tokens, channel_count),
        frozen_output_weight,
        small_weights,
        *mod_pieces,
    )
    if dense:
        keep, send, dstream, attn = dense_step(
            fsdp_index,
            seq_index,
            inputs[1],
            inputs[0],
            inputs[3],
            inputs[2],
            *inputs[4:6],
            in_order(mod_pieces, seq_index).reshape(1, -1),
            frozen_output_weight,
            small_weights,
            rank,
            scale_total,
        )
    else:
        keep, send, dstream, attn = step_call(
            inputs,
            chunks,
            spans,
            tokens,
            feature_index,
            layer_width,
            rank,
            channel_count,
            scale_total,
        )

    plane_count, plane_index = count_s // 2, seq_index // 2
    width = keep.shape[2] - 128
    half = (keep.astype(jnp.float32) + swap(send, 1).astype(jnp.float32)).astype(jnp.bfloat16)
    half = half.reshape(count_f, plane_count, rank // count_s, width + 128)
    total = pick(half, plane_index, 1).astype(jnp.float32)
    for mask in range(1, plane_count):
        total = total + swap(pick(half, plane_index ^ mask, 1), 2 * mask).astype(jnp.float32)
    margin = jnp.sum(total[0, 0, width:])
    loss = jax.nn.softplus(beta * margin).reshape(1)
    weight_pair = jax.nn.sigmoid(beta * margin)
    grad_resid = (weight_pair * dstream).astype(jnp.bfloat16).reshape(policy_residual.shape)
    grad_attn = (weight_pair * attn).astype(jnp.bfloat16).reshape(policy_attention.shape)
    pair_sum = (weight_pair * total[:, :, :width]).astype(jnp.bfloat16)
    own_sum = pick(pair_sum, fsdp_index).astype(jnp.float32)
    for step in range(1, count_f):
        arrived_sum = shift(pick(pair_sum, (fsdp_index + step) % count_f), step)
        own_sum = own_sum + arrived_sum.astype(jnp.float32)
    gathered = gather_seq(own_sum.astype(jnp.bfloat16), seq_index)
    gathered = gathered.reshape(plane_count, 2, rank // count_s, width).transpose(1, 0, 2, 3)
    sums = gathered.reshape(rank, width).astype(jnp.float32)
    square = jnp.full((8, 128), jnp.sum(sums * sums), jnp.float32)
    total_square = square
    for step in range(1, count_f):
        total_square = total_square + shift(square, step)
    upper_limit = math.sqrt(
        rank * feature_index + rank * layer_width + channel_count * layer_width
    )
    factor = jnp.minimum(1.0, upper_limit / jnp.sqrt(total_square[0, 0] + 1e-12))
    scaled = factor * sums
    return (
        loss,
        scaled[:, :down_block],
        scaled[:, down_block : down_block + block],
        scaled[:, down_block + block :],
        grad_resid,
        grad_attn,
    )


def solution(mesh):
    in_specs = (
        P("fsdp"),
        P("fsdp", None),
        P("fsdp", "seq"),
        P("fsdp", None, "seq", None),
        P("fsdp", None, "seq", None),
        P("fsdp", None, "seq", None),
        P("fsdp", None, "seq", None),
        P("fsdp", None, "seq", None),
        P("fsdp", None, "seq", None),
        P(None, "fsdp"),
        P(None, "fsdp"),
        P(None, "fsdp"),
        P(None, "fsdp"),
        P(None, "fsdp"),
    )
    out_specs = (
        P("fsdp"),
        P(None, "fsdp"),
        P(None, "fsdp"),
        P(None, "fsdp"),
        P("fsdp", None, "seq", None),
        P("fsdp", None, "seq", None),
    )

    return jax.shard_map(local, mesh=mesh, in_specs=in_specs, out_specs=out_specs, check_vma=False)
```

```python
import math

import jax
import jax.numpy as jnp
from jax import lax
from jax.experimental import pallas as pl
from jax.experimental.pallas import tpu as pltpu
from jax.sharding import PartitionSpec as P


EPSILON = 1e-06


def embedding(timestep, layer_width):
    half_width = layer_width // 2
    frequency = jnp.exp(-math.log(10000.0) * jnp.arange(half_width, dtype=jnp.float32) / half_width)
    angles = timestep.astype(jnp.float32)[:, None] * frequency[None, :]
    return jnp.concatenate([jnp.cos(angles), jnp.sin(angles)], axis=1)


def contract_rows(left, right):
    return lax.dot_general(
        left, right, (((0,), (0,)), ((), ())), preferred_element_type=jnp.float32
    )


def contracted_columns(left, right):
    return lax.dot_general(
        left, right, (((1,), (1,)), ((), ())), preferred_element_type=jnp.float32
    )


def shift(value, step):
    count = lax.axis_size("fsdp")
    return lax.ppermute(value, "fsdp", [(i, (i + step) % count) for i in range(count)])


def swap(value, mask):
    count = lax.axis_size("seq")
    return lax.ppermute(value, "seq", [(i, i ^ mask) for i in range(count)])


def pick(value, index, axis=0):
    return lax.dynamic_index_in_dim(value, index, axis, keepdims=False)


def in_order(pieces, index):
    stacked = jnp.stack(pieces)
    places = [pick(stacked, index ^ place) for place in range(len(pieces))]
    return jnp.stack(places)


def gather_seq(value, seq_index):
    count = lax.axis_size("seq")
    plane = [value] + [swap(value, 2 * mask) for mask in range(1, count // 2)]
    stacked = jnp.stack(plane)
    other = swap(stacked, 1)
    both = []
    for mask in range(count // 2):
        both += [stacked[mask], other[mask]]
    return in_order(both, seq_index)


def final_layer(projected, residual, gate_row, shift_row, scale_row, head):
    stream = residual.astype(jnp.float32) + gate_row * projected
    row_mean = jnp.mean(stream, axis=1, keepdims=True)
    centred = stream - row_mean
    variance = jnp.mean(centred * centred, axis=1, keepdims=True)
    inv_std = lax.rsqrt(variance + EPSILON)
    normed = centred * inv_std
    modulated = (normed * (1.0 + scale_row) + shift_row).astype(jnp.bfloat16)
    predicted = contracted_columns(modulated, head)
    return (normed, inv_std, modulated, predicted)


def member_errors(predicted, target, scale_total):
    offset = predicted - target
    squared = jnp.sum(offset * offset, axis=1)
    return jnp.sum(squared.reshape(2, -1), axis=1) / scale_total


def gather_weights(ext, fsdp_index, seq_index):
    rows, columns = ext.shape
    count_f, count_s = lax.axis_size("fsdp"), lax.axis_size("seq")
    part = rows // count_s
    chunk = lax.dynamic_slice(ext, (seq_index * part, 0), (part, columns))
    full = jnp.zeros((rows, columns * count_f), ext.dtype)
    full = lax.dynamic_update_slice(full, ext, (0, fsdp_index * columns))
    arrived = [shift(chunk, step) for step in range(1, count_f)]
    group = -(-len(arrived) // 3)
    for first in range(1, count_f, group):
        steps = range(first, min(first + group, count_f))
        own = jnp.concatenate([arrived[step - 1] for step in steps], axis=0)
        plane = [own] + [swap(own, 2 * mask) for mask in range(1, count_s // 2)]
        pieces = []
        for piece in plane:
            pieces += [piece, swap(piece, 1)]

        def place(at, full, piece, mask):
            row = (seq_index ^ mask) * part
            column = ((fsdp_index - first - at) % count_f) * columns
            held = lax.dynamic_slice(piece, (at * part, 0), (part, columns))
            return lax.dynamic_update_slice(full, held, (row, column))

        for mask, piece in enumerate(pieces):
            if group == 1:
                full = place(0, full, piece, mask)
            else:
                full = lax.fori_loop(
                    0, len(steps), lambda at, held: place(at, held, piece, mask), full
                )
    return full


def dot(left, right):
    return jnp.dot(left, right, preferred_element_type=jnp.float32)


def margin_lanes(filled, seq_index, rounded):
    lane = lax.broadcasted_iota(jnp.int32, filled.shape, 1) - 3 * seq_index
    high = rounded(filled)
    middle = rounded(filled - high)
    low = filled - high - middle
    return jnp.where(
        lane == 0, high, jnp.where(lane == 1, middle, jnp.where(lane == 2, low, 0.0))
    )


def step_kernel(sizes, *refs):
    tokens, features, width, rank, channels, count_f, count_s, scale_total, spans = sizes
    block, down_block = width // count_f, features // count_f
    part, small_part = features // count_s, (2 * rank + 2 * channels) // count_s
    (attn_pol, attn_ref, res_pol, res_ref, noise, latent, own, own_small), refs = refs[:8], refs[8:]
    mod_pieces, refs = refs[:count_s], refs[count_s:]
    chunks, refs = refs[: len(spans)], refs[len(spans) :]
    keep, send, dstream_out, attn_out, refs = *refs[:4], refs[4:]
    rows, base, small, residual, proj, z_hold, back, dproj, mod_hold, mod, sems = refs
    fsdp_index, seq_index = lax.axis_index("fsdp"), lax.axis_index("seq")

    def start(source, target, slot):
        copy = pltpu.make_async_copy(source, target, sems.at[slot])
        copy.start()
        return copy

    first = [
        start(attn_pol, rows.at[:tokens], 0),
        start(attn_ref, rows.at[tokens:], 1),
    ]
    blocks = [[start(own, base.at[fsdp_index], 2)]] + [[] for _ in range(1, count_f)]
    smalls = [start(own_small, small.at[fsdp_index], 3)]
    slot = 6
    for chunk, (step, mask, first_row, count) in zip(chunks, spans):
        at = lax.rem(fsdp_index - step + count_f, count_f)
        place = lax.bitwise_xor(seq_index, mask)
        wide = max(0, min(part - first_row, count))
        if wide:
            row = pl.multiple_of(place * part + first_row, 16)
            blocks[step].append(
                start(chunk.at[:wide], base.at[at, pl.ds(row, wide)], slot)
            )
        if wide < count:
            row = pl.multiple_of(place * small_part + (first_row + wide - part), 16)
            smalls.append(
                start(chunk.at[wide:], small.at[at, pl.ds(row, count - wide)], slot + 1)
            )
        slot += 2
    late = [
        start(res_pol, residual.at[:tokens], 4),
        start(res_ref, residual.at[tokens:], 5),
    ]
    for mask in range(count_s):
        place = lax.bitwise_xor(seq_index, mask)
        late.append(start(mod_pieces[mask], mod_hold.at[place], slot + mask))
    for copy in first:
        copy.wait()
    for step in [0] + shift_order(count_f):
        for copy in blocks[step]:
            copy.wait()
        at = lax.rem(fsdp_index - step + count_f, count_f)
        proj[at] = dot(rows[...], base[at])
    for copy in smalls + late:
        copy.wait()
    mod_part = mod_hold.shape[2]
    for place in range(count_s):
        mod[:, place * mod_part : (place + 1) * mod_part] = mod_hold[place]

    def up_of(g):
        return small[g, :rank]

    def head_of(g, policy):
        first_row = rank + (channels if policy else 0)
        return small[g, first_row : first_row + channels]

    def down_of(g):
        return small[g, rank + 2 * channels :, :down_block]

    def columns(g):
        return slice(g * block, (g + 1) * block)

    def gate_of(g):
        return mod[:, g * block : (g + 1) * block]

    def shift_of(g):
        return mod[:, width + g * block : width + (g + 1) * block]

    def scale_of(g):
        return 1.0 + mod[:, 2 * width + g * block : 2 * width + (g + 1) * block]

    low = jnp.zeros((tokens, rank), jnp.float32)
    for g in range(count_f):
        low = low + contracted_columns(
            rows[:tokens, g * down_block : (g + 1) * down_block], down_of(g)
        )
    low_rows = low.astype(jnp.bfloat16)
    row_sum = jnp.zeros((2 * tokens, 1), jnp.float32)
    for g in range(count_f):
        proj[g, :tokens] = proj[g, :tokens] + dot(low_rows, up_of(g))
        stream = residual[:, columns(g)].astype(jnp.float32) + gate_of(g) * proj[g]
        proj[g] = stream
        row_sum = row_sum + jnp.sum(stream, axis=1, keepdims=True)
    mean = row_sum / width
    square_sum = jnp.zeros((2 * tokens, 1), jnp.float32)
    for g in range(count_f):
        centred = proj[g] - mean
        square_sum = square_sum + jnp.sum(centred * centred, axis=1, keepdims=True)
    inv_std = lax.rsqrt(square_sum / width + EPSILON)
    pred_pol = jnp.zeros((tokens, channels), jnp.float32)
    pred_ref = jnp.zeros((tokens, channels), jnp.float32)
    for g in range(count_f):
        normed = (proj[g] - mean) * inv_std
        proj[g] = normed
        z_rows = (normed * scale_of(g) + shift_of(g)).astype(jnp.bfloat16)
        z_hold[g] = z_rows[:tokens]
        pred_pol = pred_pol + contracted_columns(z_rows[:tokens], head_of(g, True))
        pred_ref = pred_ref + contracted_columns(z_rows[tokens:], head_of(g, False))
    target = noise[...] - latent[...]
    half_rows = lax.broadcasted_iota(jnp.int32, (tokens, channels), 0) < tokens // 2
    sign = jnp.where(half_rows, 1.0, -1.0)
    off_pol, off_ref = pred_pol - target, pred_ref - target
    local_margin = jnp.sum(sign * (off_pol * off_pol - off_ref * off_ref)) / scale_total
    lanes = margin_lanes(
        jnp.full((rank // 2, 128), local_margin, jnp.float32),
        seq_index,
        lambda value: value.astype(jnp.bfloat16).astype(jnp.float32),
    ).astype(jnp.bfloat16)
    for g in range(count_f):
        keep[g, :, down_block + 2 * block :] = lanes
        send[g, :, down_block + 2 * block :] = lanes
    dpred_wide = 2.0 * sign * off_pol
    dpred = dpred_wide.astype(jnp.bfloat16)
    dpred_turned = dpred_wide.T.astype(jnp.bfloat16)
    low_turned = low.T.astype(jnp.bfloat16)
    sum_dn = jnp.zeros((tokens, 1), jnp.float32)
    sum_dn_normed = jnp.zeros((tokens, 1), jnp.float32)
    half = rank // 2
    core = lax.rem(seq_index, 2)

    def put(g, first_column, value):
        value = value.astype(jnp.bfloat16).astype(jnp.float32)
        last_column = first_column + value.shape[1]
        top, bottom = value[:half], value[half:]
        keep[g, :, first_column:last_column] = jnp.where(core == 0, top, bottom).astype(jnp.bfloat16)
        send[g, :, first_column:last_column] = jnp.where(core == 0, bottom, top).astype(jnp.bfloat16)

    for g in range(count_f):
        put(g, down_block + block, dot(dpred_turned, z_hold[g]))
        dn_rows = dot(dpred, head_of(g, True)) * scale_of(g)
        back[g] = dn_rows
        sum_dn = sum_dn + jnp.sum(dn_rows, axis=1, keepdims=True)
        sum_dn_normed = sum_dn_normed + jnp.sum(dn_rows * proj[g, :tokens], axis=1, keepdims=True)
    mean_dn, mean_dn_normed = sum_dn / width, sum_dn_normed / width
    inv_pol = inv_std[:tokens]
    low_grad = jnp.zeros((tokens, rank), jnp.float32)
    for g in range(count_f):
        dstream = inv_pol * (back[g] - mean_dn - proj[g, :tokens] * mean_dn_normed)
        dstream_out[:, columns(g)] = dstream
        dproj_rows = (gate_of(g) * dstream).astype(jnp.bfloat16)
        dproj[g] = dproj_rows
        put(g, down_block, dot(low_turned, dproj_rows))
        low_grad = low_grad + contracted_columns(dproj_rows, up_of(g))
    low_grad_rows = low_grad.astype(jnp.bfloat16)
    low_grad_turned = low_grad.T.astype(jnp.bfloat16)
    for g in range(count_f):
        put(g, 0, dot(low_grad_turned, rows[:tokens, g * down_block : (g + 1) * down_block]))
    for g in range(count_f):
        at = slice(g * down_block, (g + 1) * down_block)
        value = dot(low_grad_rows, down_of(g))
        for other in range(count_f):
            value = value + contracted_columns(dproj[other], base[other, at])
        attn_out[:, at] = value


def step_call(operands, chunks, spans, tokens, features, width, rank, channels, scale_total):
    count_f, count_s = lax.axis_size("fsdp"), lax.axis_size("seq")
    sizes = (tokens, features, width, rank, channels, count_f, count_s, scale_total, spans)
    block = width // count_f
    grads = jax.ShapeDtypeStruct(
        (count_f, rank // 2, features // count_f + 2 * block + 128), jnp.bfloat16
    )
    any_space = pl.BlockSpec(memory_space=pl.ANY)
    vmem = pl.BlockSpec(memory_space=pltpu.VMEM)
    return pl.pallas_call(
        lambda *refs: step_kernel(sizes, *refs),
        out_shape=(
            grads,
            grads,
            jax.ShapeDtypeStruct((tokens, width), jnp.float32),
            jax.ShapeDtypeStruct((tokens, features), jnp.float32),
        ),
        in_specs=[any_space] * 4
        + [vmem] * 2
        + [any_space] * (len(operands) - 6 + len(chunks)),
        out_specs=(vmem,) * 4,
        scratch_shapes=[
            pltpu.VMEM((2 * tokens, features), jnp.bfloat16),
            pltpu.VMEM((count_f, features, block), jnp.bfloat16),
            pltpu.VMEM((count_f, 2 * rank + 2 * channels, block), jnp.bfloat16),
            pltpu.VMEM((2 * tokens, width), jnp.bfloat16),
            pltpu.VMEM((count_f, 2 * tokens, block), jnp.float32),
            pltpu.VMEM((count_f, tokens, block), jnp.bfloat16),
            pltpu.VMEM((count_f, tokens, block), jnp.float32),
            pltpu.VMEM((count_f, tokens, block), jnp.bfloat16),
            pltpu.VMEM((count_s, 1, 3 * width // count_s), jnp.float32),
            pltpu.VMEM((1, 3 * width), jnp.float32),
            pltpu.SemaphoreType.DMA((6 + 2 * len(chunks) + count_s,)),
        ],
        compiler_params=pltpu.CompilerParams(vmem_limit_bytes=60 * 1024 * 1024),
        name="step",
    )(*operands, *chunks)


def shift_order(count_f):
    return sorted(range(1, count_f), key=lambda step: step * (count_f - step))


def send_chunks(own, own_small, seq_index):
    count_f, count_s = lax.axis_size("fsdp"), lax.axis_size("seq")
    part, small_part = own.shape[0] // count_s, own_small.shape[0] // count_s
    columns = own.shape[1]
    chunk = jnp.concatenate(
        [
            lax.dynamic_slice(own, (seq_index * part, 0), (part, columns)),
            lax.dynamic_slice(own_small, (seq_index * small_part, 0), (small_part, columns)),
        ],
        axis=0,
    )
    arrived = []
    for step in shift_order(count_f):
        arrived.append(shift(chunk, step))
    return arrived


def spread_chunks(arrived, part, small_part):
    count_f, count_s = lax.axis_size("fsdp"), lax.axis_size("seq")
    middle = (part + small_part) // 32 * 16
    chunks, spans = [], []

    def add(mask, first_row, piece):
        chunks.extend([piece, swap(piece, 1)])
        spans.append((step, mask, first_row, piece.shape[0]))
        spans.append((step, mask + 1, first_row, piece.shape[0]))

    for number, step in enumerate(shift_order(count_f), 1):
        held = arrived[number - 1]
        add(0, 0, held)
        if count_s == 8:
            first, second = swap(held, 2), swap(held, 4)
            top, bottom = swap(first[:middle], 4), swap(second[middle:], 2)
            add(2, 0, first)
            add(4, 0, second)
            add(6, 0, top)
            add(6, middle, bottom)
        else:
            for mask in range(2, count_s, 2):
                add(mask, 0, swap(held, mask))
    return chunks, tuple(spans)


def dense_step(
    fsdp_index,
    seq_index,
    reference_attention,
    policy_attention,
    reference_residual,
    policy_residual,
    noise,
    latent,
    modulation,
    frozen_output_weight,
    small_weights,
    rank,
    scale_total,
):
    feature_index, block = frozen_output_weight.shape
    tokens, layer_width = reference_residual.shape
    channel_count = noise.shape[1]
    count_f = lax.axis_size("fsdp")
    down_block = feature_index // count_f
    gate_row = modulation[:, :layer_width]
    shift_row = modulation[:, layer_width : 2 * layer_width]
    scale_row = modulation[:, 2 * layer_width :]
    ext = jnp.concatenate([frozen_output_weight, small_weights], axis=0)
    full = gather_weights(ext, fsdp_index, seq_index)
    base_full = full[:feature_index]
    up_full = full[feature_index : feature_index + rank]
    head_ref_full = full[feature_index + rank : feature_index + rank + channel_count]
    head_pol_full = full[feature_index + rank + channel_count : feature_index + rank + 2 * channel_count]
    down_full = (
        full[feature_index + rank + 2 * channel_count :]
        .reshape(rank, count_f, block)[:, :, :down_block]
        .reshape(rank, feature_index)
    )

    rows_ref, policy_rows = reference_attention, policy_attention
    stream_ref, stream_pol = reference_residual, policy_residual
    target = noise - latent
    tok_seq = tokens // 2
    sign_rows = jnp.concatenate(
        [jnp.ones((tok_seq, 1), jnp.float32), -jnp.ones((tok_seq, 1), jnp.float32)], axis=0
    )
    proj_ref = jnp.dot(rows_ref, base_full, preferred_element_type=jnp.float32)
    _, _, _, pred_ref = final_layer(
        proj_ref, stream_ref, gate_row, shift_row, scale_row, head_ref_full
    )
    part_ref = member_errors(pred_ref, target, scale_total)
    low_rank_rows = contracted_columns(policy_rows, down_full).astype(jnp.bfloat16)
    policy_projection = jnp.dot(
        policy_rows, base_full, preferred_element_type=jnp.float32
    ) + jnp.dot(low_rank_rows, up_full, preferred_element_type=jnp.float32)
    normed_pol, inv_pol, z_pol, pred_pol = final_layer(
        policy_projection, stream_pol, gate_row, shift_row, scale_row, head_pol_full
    )
    part_pol = member_errors(pred_pol, target, scale_total)
    local_margin = part_pol[0] - part_ref[0] - (part_pol[1] - part_ref[1])
    lanes = margin_lanes(
        jnp.full((rank, 128), local_margin, jnp.float32),
        seq_index,
        lambda value: lax.reduce_precision(value, 8, 7),
    ).astype(jnp.bfloat16)

    dpred = (sign_rows * 2.0 * (pred_pol - target)).astype(jnp.bfloat16)
    head_part = contract_rows(dpred, z_pol)
    dz_rows = jnp.dot(dpred, head_pol_full, preferred_element_type=jnp.float32)
    dn_rows = dz_rows * (1.0 + scale_row)
    dstream = inv_pol * (
        dn_rows
        - jnp.mean(dn_rows, axis=1, keepdims=True)
        - normed_pol * jnp.mean(dn_rows * normed_pol, axis=1, keepdims=True)
    )
    projection_gradient = (gate_row * dstream).astype(jnp.bfloat16)
    up_part = contract_rows(low_rank_rows, projection_gradient)
    low_rank_gradient = contracted_columns(projection_gradient, up_full).astype(jnp.bfloat16)
    down_part = contract_rows(low_rank_gradient, policy_rows)
    attn = contracted_columns(projection_gradient, base_full) + jnp.dot(
        low_rank_gradient, down_full, preferred_element_type=jnp.float32
    )

    def blocks(value):
        return value.astype(jnp.bfloat16).reshape(value.shape[0], count_f, -1).transpose(1, 0, 2)

    lanes = jnp.broadcast_to(lanes[None], (count_f,) + lanes.shape)
    grads = jnp.concatenate([blocks(down_part), blocks(up_part), blocks(head_part), lanes], axis=2)
    grads = grads.reshape(count_f, 2, rank // 2, -1)
    core = seq_index % 2
    return (pick(grads, core, 1), pick(grads, 1 - core, 1), dstream, attn)


def local(
    timestep,
    pooled,
    modulation_weight,
    reference_attention,
    policy_attention,
    reference_residual,
    policy_residual,
    noise,
    latent,
    frozen_output_weight,
    adapter_down_weight,
    adapter_up_weight,
    reference_head,
    policy_head,
):
    layer_width = pooled.shape[1]
    feature_index = reference_attention.shape[-1]
    channel_count = noise.shape[-1]
    rank = adapter_down_weight.shape[0]
    tok_seq = reference_attention.shape[2]
    count_f, count_s = lax.axis_size("fsdp"), lax.axis_size("seq")
    fsdp_index, seq_index = lax.axis_index("fsdp"), lax.axis_index("seq")
    length = tok_seq * count_s
    scale_total = float(length * channel_count)
    beta = math.sqrt(length * channel_count) / 8.0

    block = frozen_output_weight.shape[1]
    down_block = adapter_down_weight.shape[1]
    small_weights = jnp.concatenate(
        [
            adapter_up_weight,
            reference_head,
            policy_head,
            jnp.pad(adapter_down_weight, ((0, 0), (0, block - down_block))),
        ],
        axis=0,
    )
    part, small_part = feature_index // count_s, small_weights.shape[0] // count_s
    dense = down_block % 128 or block % 128 or part % 16 or small_part % 16 or rank % 32
    if not dense:
        arrived = send_chunks(frozen_output_weight, small_weights, seq_index)
        chunks, spans = spread_chunks(arrived, part, small_part)

    cond_vec = pooled.astype(jnp.float32) + embedding(timestep, layer_width)
    activated = jax.nn.silu(cond_vec).astype(jnp.bfloat16)
    by_block = activated.reshape(pooled.shape[0], count_f, -1).transpose(1, 0, 2)
    pieces = [pick(by_block, fsdp_index)]
    for step in range(1, count_f):
        pieces.append(shift(pick(by_block, (fsdp_index + step) % count_f), step))
    per_pair = pooled.shape[0]
    if not dense:
        late = [at for at, (step, mask, *_) in enumerate(spans) if (step, mask) == (1, 2)]
        pieces = lax.optimization_barrier((pieces, chunks[late[0]] if late else arrived[0]))[0]
    partial_value = jnp.dot(
        jnp.concatenate(pieces, axis=0), modulation_weight, preferred_element_type=jnp.float32
    )
    own_part = partial_value[:per_pair]
    for step in range(1, count_f):
        own_part = own_part + shift(
            partial_value[per_pair * step : per_pair * (step + 1)], count_f - step
        )
    mod_plane = [own_part] + [swap(own_part, 2 * mask) for mask in range(1, count_s // 2)]
    mod_pieces = []
    for piece in mod_plane:
        mod_pieces += [piece, swap(piece, 1)]

    tokens = 2 * tok_seq
    inputs = (
        policy_attention.reshape(tokens, feature_index),
        reference_attention.reshape(tokens, feature_index),
        policy_residual.reshape(tokens, layer_width),
        reference_residual.reshape(tokens, layer_width),
        noise.reshape(tokens, channel_count),
        latent.reshape(tokens, channel_count),
        frozen_output_weight,
        small_weights,
        *mod_pieces,
    )
    if dense:
        keep, send, dstream, attn = dense_step(
            fsdp_index,
            seq_index,
            inputs[1],
            inputs[0],
            inputs[3],
            inputs[2],
            *inputs[4:6],
            in_order(mod_pieces, seq_index).reshape(1, -1),
            frozen_output_weight,
            small_weights,
            rank,
            scale_total,
        )
    else:
        keep, send, dstream, attn = step_call(
            inputs,
            chunks,
            spans,
            tokens,
            feature_index,
            layer_width,
            rank,
            channel_count,
            scale_total,
        )

    plane_count, plane_index = count_s // 2, seq_index // 2
    width = keep.shape[2] - 128
    half = (keep.astype(jnp.float32) + swap(send, 1).astype(jnp.float32)).astype(jnp.bfloat16)
    half = half.reshape(count_f, plane_count, rank // count_s, width + 128)
    total = pick(half, plane_index, 1).astype(jnp.float32)
    for mask in range(1, plane_count):
        total = total + swap(pick(half, plane_index ^ mask, 1), 2 * mask).astype(jnp.float32)
    margin = jnp.sum(total[0, 0, width:])
    loss = jax.nn.softplus(beta * margin).reshape(1)
    weight_pair = jax.nn.sigmoid(beta * margin)
    grad_resid = (weight_pair * dstream).astype(jnp.bfloat16).reshape(policy_residual.shape)
    grad_attn = (weight_pair * attn).astype(jnp.bfloat16).reshape(policy_attention.shape)
    pair_sum = (weight_pair * total[:, :, :width]).astype(jnp.bfloat16)
    own_sum = pick(pair_sum, fsdp_index).astype(jnp.float32)
    for step in range(1, count_f):
        arrived_sum = shift(pick(pair_sum, (fsdp_index + step) % count_f), step)
        own_sum = own_sum + arrived_sum.astype(jnp.float32)
    gathered = gather_seq(own_sum.astype(jnp.bfloat16), seq_index)
    gathered = gathered.reshape(plane_count, 2, rank // count_s, width).transpose(1, 0, 2, 3)
    sums = gathered.reshape(rank, width).astype(jnp.float32)
    square = jnp.full((8, 128), jnp.sum(sums * sums), jnp.float32)
    total_square = square
    for step in range(1, count_f):
        total_square = total_square + shift(square, step)
    upper_limit = math.sqrt(
        rank * feature_index + rank * layer_width + channel_count * layer_width
    )
    factor = jnp.minimum(1.0, upper_limit / jnp.sqrt(total_square[0, 0] + 1e-12))
    scaled = factor * sums
    return (
        loss,
        scaled[:, :down_block],
        scaled[:, down_block : down_block + block],
        scaled[:, down_block + block :],
        grad_resid,
        grad_attn,
    )


def solution(mesh):
    in_specs = (
        P("fsdp"),
        P("fsdp", None),
        P("fsdp", "seq"),
        P("fsdp", None, "seq", None),
        P("fsdp", None, "seq", None),
        P("fsdp", None, "seq", None),
        P("fsdp", None, "seq", None),
        P("fsdp", None, "seq", None),
        P("fsdp", None, "seq", None),
        P(None, "fsdp"),
        P(None, "fsdp"),
        P(None, "fsdp"),
        P(None, "fsdp"),
        P(None, "fsdp"),
    )
    out_specs = (
        P("fsdp"),
        P(None, "fsdp"),
        P(None, "fsdp"),
        P(None, "fsdp"),
        P("fsdp", None, "seq", None),
        P("fsdp", None, "seq", None),
    )

    return jax.shard_map(local, mesh=mesh, in_specs=in_specs, out_specs=out_specs, check_vma=False)
```
